16 devices in a mesh: dp: 4 (over z, y), pp: 4 (over x, core).
Axes of the slice: x: 2, y: 2, z: 2, core: 2. Of those that a mesh axis runs over, the one named last changes fastest.
Arguments:
- tokens: int32 [2, 32, 34], P(None, 'dp')
- emb_s: float32 [4, 32128, 1024], P('pp', 'dp')
- w_up: bfloat16 [4, 1, 1024, 4096], P('pp')
- w_down: bfloat16 [4, 1, 4096, 1024], P('pp')
- gain_f: bfloat16 [1024], replicated
- gain_h: bfloat16 [1024], replicated
- gain_e: bfloat16 [1024], replicated
- gain_m: bfloat16 [1024], replicated
- w_proj: bfloat16 [2048, 1024], replicated
- u_up: bfloat16 [1024, 4096], replicated
- u_down: bfloat16 [4096, 1024], replicated
Outputs:
- output 1: float32 [], replicated
- output 2: float32 [4, 32128, 1024], P('pp', 'dp')
- output 3: float32 [4, 1, 1024, 4096], P('pp')
- output 4: float32 [4, 1, 4096, 1024], P('pp')
All inputs are finite; a program needn't handle non-finite values.
Results may differ from the reference program's by a relative error of at most 0.0185332.
Values are sent between devices in bfloat16 or wider.
A program may use at most 1 GiB of HBM per device.

```python
import math
import jax
import jax.numpy as jnp
from jax import lax

PP_SIZE = 4
DP_SIZE = 4
MICRO = 2
BATCH_DEV = 8
SEQ = 32
LAYERS = 1
HIDDEN = 1024
FFN = 4096
VOCAB = 32128
BATCH = DP_SIZE * BATCH_DEV
BLOCK_TOKENS = BATCH_DEV * SEQ
MTP_WEIGHT = 0.3
EPS = 1e-6
EMB_SCALE = math.sqrt(HIDDEN)


def setup_inputs(seed: int = 0) -> dict:
    rand_keys = jax.random.split(jax.random.key(seed), 12)
    tokens = jax.random.randint(rand_keys[0], (MICRO, BATCH, SEQ + 2), 0, VOCAB, dtype=jnp.int32)
    tokens = tokens.at[0, 0, 0].set(0).at[0, 0, 1].set(VOCAB - 1)
    emb_full = jax.random.normal(rand_keys[1], (VOCAB, HIDDEN), jnp.float32) * HIDDEN ** -0.5
    emb_s = jnp.concatenate([emb_full[None], jnp.zeros((PP_SIZE - 1, VOCAB, HIDDEN), jnp.float32)], axis=0)
    w_up = (jax.random.normal(rand_keys[2], (PP_SIZE, LAYERS, HIDDEN, FFN), jnp.float32) * HIDDEN ** -0.5).astype(jnp.bfloat16)
    w_down = (jax.random.normal(rand_keys[3], (PP_SIZE, LAYERS, FFN, HIDDEN), jnp.float32) * FFN ** -0.5).astype(jnp.bfloat16)
    gain_f = (1.0 + 0.3 * jax.random.normal(rand_keys[4], (HIDDEN,), jnp.float32)).astype(jnp.bfloat16)
    gain_h = (1.0 + 0.3 * jax.random.normal(rand_keys[5], (HIDDEN,), jnp.float32)).astype(jnp.bfloat16)
    gain_e = (1.0 + 0.3 * jax.random.normal(rand_keys[6], (HIDDEN,), jnp.float32)).astype(jnp.bfloat16)
    gain_m = (1.0 + 0.3 * jax.random.normal(rand_keys[7], (HIDDEN,), jnp.float32)).astype(jnp.bfloat16)
    w_proj = (jax.random.normal(rand_keys[8], (2 * HIDDEN, HIDDEN), jnp.float32) * (2 * HIDDEN) ** -0.5).astype(jnp.bfloat16)
    u_up = (jax.random.normal(rand_keys[9], (HIDDEN, FFN), jnp.float32) * HIDDEN ** -0.5).astype(jnp.bfloat16)
    u_down = (jax.random.normal(rand_keys[10], (FFN, HIDDEN), jnp.float32) * FFN ** -0.5).astype(jnp.bfloat16)
    return dict(tokens=tokens, emb_s=emb_s, w_up=w_up, w_down=w_down, gain_f=gain_f, gain_h=gain_h, gain_e=gain_e, gain_m=gain_m, w_proj=w_proj, u_up=u_up, u_down=u_down)


def norm_only(acts):
    acts_f = acts.astype(jnp.float32)
    return acts_f * lax.rsqrt(jnp.mean(acts_f * acts_f, axis=-1, keepdims=True) + EPS)


def gain_norm(acts, gain):
    return (norm_only(acts) * gain.astype(jnp.float32)).astype(jnp.bfloat16)


def lookup_rows(emb_full, tok_ids):
    return (emb_full[tok_ids].astype(jnp.bfloat16).astype(jnp.float32) * EMB_SCALE).astype(jnp.bfloat16)


def cross_sum(normed, emb_table, targets):
    logits = jnp.dot(normed, emb_table.T, preferred_element_type=jnp.float32)
    row_max = lax.stop_gradient(jnp.max(logits, axis=-1, keepdims=True))
    log_norm = jnp.log(jnp.sum(jnp.exp(logits - row_max), axis=-1)) + row_max[:, 0]
    picked = jnp.take_along_axis(logits, targets[:, None], axis=-1)[:, 0]
    return jnp.sum(log_norm - picked)


def trunk_layer(acts, layer_weights):
    w_in, w_out = layer_weights
    normed = norm_only(acts).astype(jnp.bfloat16)
    act_out = jax.nn.gelu(jnp.dot(normed, w_in.astype(jnp.bfloat16), preferred_element_type=jnp.float32)).astype(jnp.bfloat16)
    layer_out = (acts.astype(jnp.float32) + jnp.dot(act_out, w_out.astype(jnp.bfloat16), preferred_element_type=jnp.float32)).astype(jnp.bfloat16)
    return layer_out, None


def block_loss(emb_full, flat_up, flat_down, tok_ids, extras):
    gain_f, gain_h, gain_e, gain_m, w_proj, u_up, u_down = extras
    emb_table = emb_full.astype(jnp.bfloat16)
    in_ids = tok_ids[:, 0:SEQ].reshape(BLOCK_TOKENS)
    mid_ids = tok_ids[:, 1:SEQ + 1].reshape(BLOCK_TOKENS)
    out_ids = tok_ids[:, 2:SEQ + 2].reshape(BLOCK_TOKENS)
    hidden_out, _ = lax.scan(trunk_layer, lookup_rows(emb_full, in_ids), (flat_up, flat_down))
    main_sum = cross_sum(gain_norm(hidden_out, gain_f), emb_table, mid_ids)
    mtp_rows = lookup_rows(emb_full, mid_ids)
    joined = jnp.concatenate([gain_norm(hidden_out, gain_h), gain_norm(mtp_rows, gain_e)], axis=-1)
    mtp_state = jnp.dot(joined, w_proj, preferred_element_type=jnp.float32).astype(jnp.bfloat16)
    mtp_inner = jax.nn.gelu(jnp.dot(gain_norm(mtp_state, gain_m), u_up, preferred_element_type=jnp.float32)).astype(jnp.bfloat16)
    mtp_state = (mtp_state.astype(jnp.float32) + jnp.dot(mtp_inner, u_down, preferred_element_type=jnp.float32)).astype(jnp.bfloat16)
    next_sum = cross_sum(gain_norm(mtp_state, gain_f), emb_table, out_ids)
    return (main_sum + MTP_WEIGHT * next_sum) / (MICRO * BATCH * SEQ)


def reference(tokens, emb_s, w_up, w_down, gain_f, gain_h, gain_e, gain_m, w_proj, u_up, u_down):
    extras = (gain_f, gain_h, gain_e, gain_m, w_proj, u_up, u_down)
    emb_full = emb_s[0]
    flat_up = w_up.astype(jnp.float32).reshape(PP_SIZE * LAYERS, HIDDEN, FFN)
    flat_down = w_down.astype(jnp.float32).reshape(PP_SIZE * LAYERS, FFN, HIDDEN)
    blocks = tokens.reshape(MICRO * DP_SIZE, BATCH_DEV, SEQ + 2)
    grad_fn = jax.value_and_grad(block_loss, argnums=(0, 1, 2))

    def block_step(carry, tok_ids):
        loss_acc, g_emb, g_up, g_down = carry
        value, grads = grad_fn(emb_full, flat_up, flat_down, tok_ids, extras)
        return (loss_acc + value, g_emb + grads[0], g_up + grads[1], g_down + grads[2]), None

    start_carry = (jnp.zeros((), jnp.float32), jnp.zeros_like(emb_full), jnp.zeros_like(flat_up), jnp.zeros_like(flat_down))
    (loss, g_emb, g_up, g_down), _ = lax.scan(block_step, start_carry, blocks)
    d_emb_s = jnp.concatenate([g_emb[None], jnp.zeros((PP_SIZE - 1, VOCAB, HIDDEN), jnp.float32)], axis=0)
    return loss, d_emb_s, g_up.reshape(PP_SIZE, LAYERS, HIDDEN, FFN), g_down.reshape(PP_SIZE, LAYERS, FFN, HIDDEN)
```

```python
import math
import jax
import jax.numpy as jnp
from jax import lax
from jax.experimental import pallas as pl
from jax.experimental.pallas import tpu as pltpu
from jax.sharding import PartitionSpec as P

MTP_WEIGHT = 0.3
EPS = 1e-6
BF = jnp.bfloat16
F32 = jnp.float32


def norm_only(acts):
    acts_f = acts.astype(F32)
    return acts_f * lax.rsqrt(jnp.mean(acts_f * acts_f, axis=-1, keepdims=True) + EPS)


def norm_bf16(acts):
    return norm_only(acts).astype(BF)


def gain_norm(acts, gain):
    return (norm_only(acts) * gain.astype(F32)).astype(BF)


def gelu_bf16(pre_act):
    return jax.nn.gelu(pre_act).astype(BF)


def dot(a, b, dims):
    return lax.dot_general(a, b, (dims, ((), ())), preferred_element_type=F32)


def normed_heads(hid, rows, gain_f, gain_h, gain_e, gain_m, w_proj, u_up, u_down):
    main = gain_norm(hid, gain_f)
    joined = jnp.concatenate([gain_norm(hid, gain_h), gain_norm(rows, gain_e)], axis=-1)
    state = jnp.dot(joined, w_proj, preferred_element_type=F32).astype(BF)
    inner = gelu_bf16(jnp.dot(gain_norm(state, gain_m), u_up, preferred_element_type=F32))
    state = (state.astype(F32) + jnp.dot(inner, u_down, preferred_element_type=F32)).astype(BF)
    return main, gain_norm(state, gain_f)


def stage_fwd(acts, w_in, w_out):
    act_out = gelu_bf16(jnp.dot(norm_bf16(acts), w_in, preferred_element_type=F32))
    return (acts.astype(F32) + jnp.dot(act_out, w_out, preferred_element_type=F32)).astype(BF)


def stage_dgrad(acts, w_in, w_out, d_out):
    normed, norm_back = jax.vjp(norm_bf16, acts)
    pre_act = jnp.dot(normed, w_in, preferred_element_type=F32)
    _, gelu_back = jax.vjp(gelu_bf16, pre_act)
    d_act = dot(d_out, w_out, ((1,), (1,))).astype(BF)
    d_pre = gelu_back(d_act)[0].astype(BF)
    d_norm = dot(d_pre, w_in, ((1,), (1,))).astype(BF)
    return (d_out.astype(F32) + norm_back(d_norm)[0].astype(F32)).astype(BF)


def stage_wgrad(acts, w_in, w_out, d_out):
    normed = norm_bf16(acts)
    pre_act = jnp.dot(normed, w_in, preferred_element_type=F32)
    act_out, gelu_back = jax.vjp(gelu_bf16, pre_act)
    g_out = dot(act_out, d_out, ((0,), (0,)))
    d_act = dot(d_out, w_out, ((1,), (1,))).astype(BF)
    d_pre = gelu_back(d_act)[0].astype(BF)
    g_in = dot(normed, d_pre, ((0,), (0,)))
    return g_in, g_out


TILE = 256


def scatter_kernel(starts_ref, rows_ref, perm_ref, base_ref, upd_ref, out_ref):
    tile = pl.program_id(0)
    out_ref[...] = base_ref[...]

    def add_row(k, carry):
        row = rows_ref[k] - tile * TILE
        out_ref[pl.ds(row, 1), :] += upd_ref[pl.ds(perm_ref[k], 1), :]
        return carry

    lax.fori_loop(starts_ref[tile], starts_ref[tile + 1], add_row, 0)


def scatter_rows(base, upd, ids):
    n_rows, hidden = base.shape
    n_tiles = pl.cdiv(n_rows, TILE)
    n_upd = ids.shape[0]
    sorted_ids, perm = lax.sort((ids, lax.iota(jnp.int32, n_upd)), num_keys=1)
    bounds = jnp.minimum(jnp.arange(n_tiles + 1, dtype=jnp.int32) * TILE, n_rows)
    starts = jnp.sum((ids[None, :] < bounds[:, None]).astype(jnp.int32), axis=1)
    return pl.pallas_call(
        scatter_kernel,
        grid_spec=pltpu.PrefetchScalarGridSpec(
            num_scalar_prefetch=3,
            grid=(n_tiles,),
            in_specs=[pl.BlockSpec((TILE, hidden), lambda i, *_: (i, 0)), pl.BlockSpec(memory_space=pltpu.VMEM)],
            out_specs=pl.BlockSpec((TILE, hidden), lambda i, *_: (i, 0)),
        ),
        out_shape=jax.ShapeDtypeStruct(base.shape, F32),
        name='scatter_rows',
    )(starts, sorted_ids, perm, base, upd)


def solution(mesh):
    n_stages = mesh.shape['pp']
    n_data = mesh.shape['dp']
    fwd_perm = [(i, i + 1) for i in range(n_stages - 1)]
    bwd_perm = [(i + 1, i) for i in range(n_stages - 1)]
    both = ('dp', 'pp')

    def from_first(pieces, stage):
        mine = jnp.where(stage == 0, pieces[0], jnp.zeros_like(pieces[0]))
        for q in range(1, n_stages):
            mine = mine + lax.ppermute(pieces[q], 'pp', [(0, q)])
        return mine

    def device_step(tokens, emb_s, w_up, w_down, gain_f, gain_h, gain_e, gain_m, w_proj, u_up, u_down):
        stage = lax.axis_index('pp')
        data = lax.axis_index('dp')
        is_first = stage == 0
        is_last = stage == n_stages - 1
        n_micro, rows_dev, width = tokens.shape
        seq_len = width - 2
        n_tok = rows_dev * seq_len
        n_own = n_micro * n_tok
        n_all = n_own * n_data
        table = emb_s[0]
        v_own, hidden = table.shape
        v_dev = v_own // n_stages
        n_vocab = v_own * n_data
        emb_scale = math.sqrt(hidden)
        loss_scale = 1.0 / n_all
        w_in = w_up[0, 0]
        w_out = w_down[0, 0]
        n_seq = n_micro * rows_dev
        q_seq = n_seq // n_stages
        n_q = q_seq * seq_len

        tok_all = lax.all_gather(tokens.reshape(n_seq, width), 'dp', axis=0, tiled=True)
        local_ids = tok_all.reshape(-1) - data * v_own
        owned = (local_ids >= 0) & (local_ids < v_own)
        got = jnp.take(table, jnp.clip(local_ids, 0, v_own - 1), axis=0)
        got = jnp.where(owned[:, None], got, 0.0).astype(BF)
        rows = lax.psum_scatter(got, 'dp', scatter_dimension=0, tiled=True)
        rows = rows.reshape(n_seq, width, hidden)

        table_q = from_first([table[q * v_dev:(q + 1) * v_dev].astype(BF) for q in range(n_stages)], stage)
        rows_q = from_first([rows[q * q_seq:(q + 1) * q_seq] for q in range(n_stages)], stage)

        first_in = (rows[:, 0:seq_len].astype(F32) * emb_scale).astype(BF).reshape(n_micro, n_tok, hidden)
        n_ticks = n_micro + n_stages - 1
        stage_in = jnp.zeros((n_micro, n_tok, hidden), BF)
        stage_out = jnp.zeros((n_micro, n_tok, hidden), BF)
        received = jnp.zeros((n_tok, hidden), BF)
        for tick in range(n_ticks):
            slot = tick - stage
            valid = (slot >= 0) & (slot < n_micro)
            slot_safe = jnp.clip(slot, 0, n_micro - 1)
            own_in = first_in[min(tick, n_micro - 1)]
            acts_in = jnp.where(is_first, own_in, received)
            acts_out = stage_fwd(acts_in, w_in, w_out)
            old_in = lax.dynamic_index_in_dim(stage_in, slot_safe, 0, keepdims=False)
            stage_in = lax.dynamic_update_index_in_dim(stage_in, jnp.where(valid, acts_in, old_in), slot_safe, 0)
            old_out = lax.dynamic_index_in_dim(stage_out, slot_safe, 0, keepdims=False)
            stage_out = lax.dynamic_update_index_in_dim(stage_out, jnp.where(valid, acts_out, old_out), slot_safe, 0)
            if tick < n_ticks - 1:
                received = lax.ppermute(acts_out, 'pp', fwd_perm)

        acts_all = lax.all_gather(stage_in.reshape(n_own, hidden), 'dp', axis=0, tiled=True)

        hid_flat = stage_out.reshape(n_own, hidden)
        hid_q = jnp.where(is_last, hid_flat[(n_stages - 1) * n_q:], jnp.zeros((n_q, hidden), BF))
        for q in range(n_stages - 1):
            hid_q = hid_q + lax.ppermute(hid_flat[q * n_q:(q + 1) * n_q], 'pp', [(n_stages - 1, q)])
        mtp_rows = (rows_q[:, 1:seq_len + 1].astype(F32) * emb_scale).astype(BF).reshape(n_q, hidden)

        def heads(hid, mtp):
            return normed_heads(hid, mtp, gain_f, gain_h, gain_e, gain_m, w_proj, u_up, u_down)

        (main_q, next_q), heads_back = jax.vjp(heads, hid_q, mtp_rows)

        dev_index = data * n_stages + stage
        shard_base = data * v_own + stage * v_dev
        columns = lax.broadcasted_iota(jnp.int32, (n_all, v_dev), 1)

        def head_fwd(norm_q):
            norm_all = lax.all_gather(norm_q, both, axis=0, tiled=True)
            logits = dot(norm_all, table_q, ((1,), (1,)))
            top = jnp.max(logits, axis=-1)
            total = jnp.sum(jnp.exp(logits - top[:, None]), axis=-1)
            stats = lax.all_gather(jnp.stack([top, total]), both, axis=0)
            top_all = jnp.max(stats[:, 0], axis=0)
            sum_all = jnp.sum(stats[:, 1] * jnp.exp(stats[:, 0] - top_all[None]), axis=0)
            return norm_all, logits, jnp.log(sum_all) + top_all

        def head_bwd(norm_all, logits, log_norm, targets, weight):
            hit = columns == (targets - shard_base)[:, None]
            d_logits = ((jnp.exp(logits - log_norm[:, None]) - hit.astype(F32)) * weight).astype(BF)
            d_norm = lax.psum_scatter(dot(d_logits, table_q, ((1,), (0,))), both, scatter_dimension=0, tiled=True)
            return d_norm.astype(BF), dot(d_logits, norm_all, ((0,), (0,)))

        mid_all = tok_all[:, 1:seq_len + 1].reshape(n_all)
        out_all = tok_all[:, 2:seq_len + 2].reshape(n_all)
        main_all, main_logits, main_lse = head_fwd(main_q)
        next_all, next_logits, next_lse = head_fwd(next_q)
        d_next, g_next = head_bwd(next_all, next_logits, next_lse, out_all, MTP_WEIGHT * loss_scale)
        d_main, g_main = head_bwd(main_all, main_logits, main_lse, mid_all, loss_scale)
        g_table = g_main + g_next

        def own(lse):
            return lax.dynamic_slice(lse, (dev_index * n_q,), (n_q,))

        mid_rows = rows_q[:, 1:seq_len + 1].reshape(n_q, hidden).astype(F32)
        out_rows = rows_q[:, 2:seq_len + 2].reshape(n_q, hidden).astype(F32)
        main_pick = jnp.sum(main_q.astype(F32) * mid_rows, axis=-1)
        next_pick = jnp.sum(next_q.astype(F32) * out_rows, axis=-1)
        local_loss = (jnp.sum(own(main_lse) - main_pick) + MTP_WEIGHT * jnp.sum(own(next_lse) - next_pick)) * loss_scale
        loss = lax.psum(local_loss, both)

        d_hid_q, d_rows_q = heads_back((d_main, d_next))
        d_rows_all = lax.all_gather(d_rows_q, both, axis=0, tiled=True)

        d_top = [lax.ppermute(d_hid_q, 'pp', [(q, n_stages - 1)]) for q in range(n_stages - 1)] + [d_hid_q]
        d_top = jnp.concatenate(d_top, axis=0).reshape(n_micro, n_tok, hidden)

        d_outs = jnp.zeros((n_micro, n_tok, hidden), BF)
        d_first = []
        received = jnp.zeros((n_tok, hidden), BF)
        for tick in range(n_ticks):
            slot = tick - (n_stages - 1 - stage)
            valid = (slot >= 0) & (slot < n_micro)
            slot_safe = jnp.clip(slot, 0, n_micro - 1)
            d_out = jnp.where(is_last, d_top[min(tick, n_micro - 1)], received)
            acts_in = lax.dynamic_index_in_dim(stage_in, slot_safe, 0, keepdims=False)
            old_d = lax.dynamic_index_in_dim(d_outs, slot_safe, 0, keepdims=False)
            d_outs = lax.dynamic_update_index_in_dim(d_outs, jnp.where(valid, d_out, old_d), slot_safe, 0)
            d_in = stage_dgrad(acts_in, w_in, w_out, d_out)
            if tick >= n_stages - 1:
                d_first.append(d_in)
            if tick < n_ticks - 1:
                received = lax.ppermute(d_in, 'pp', bwd_perm)
        d_out_all = lax.all_gather(d_outs.reshape(n_own, hidden), 'dp', axis=0, tiled=True)
        g_in, g_out = stage_wgrad(acts_all, w_in, w_out, d_out_all)

        d_first_all = lax.all_gather(jnp.concatenate(d_first, axis=0), 'dp', axis=0, tiled=True)
        seqs = n_seq * n_data
        upd = jnp.pad(d_first_all.reshape(seqs, seq_len, hidden), ((0, 0), (0, 1), (0, 0))).astype(F32)
        upd = upd + jnp.pad(d_rows_all.reshape(seqs, seq_len, hidden), ((0, 0), (1, 0), (0, 0))).astype(F32)
        upd = (upd * emb_scale).reshape(seqs * (seq_len + 1), hidden)
        pieces = [jnp.where(is_first, g_table, 0.0)]
        for q in range(1, n_stages):
            pieces.append(lax.ppermute(g_table, 'pp', [(q, 0)]))
        base = jnp.concatenate(pieces, axis=0)
        look_ids = jnp.where(is_first, tok_all[:, 0:seq_len + 1].reshape(-1) - data * v_own, -1)
        look_ids = jnp.where((look_ids >= 0) & (look_ids < v_own), look_ids, n_vocab)
        g_shard = scatter_rows(base, upd, look_ids)
        return loss, g_shard[None], g_in[None, None], g_out[None, None]

    return jax.shard_map(device_step, mesh=mesh, in_specs=(P(None, 'dp', None), P('pp', 'dp', None), P('pp'), P('pp'), P(), P(), P(), P(), P(), P(), P()), out_specs=(P(), P('pp', 'dp', None), P('pp'), P('pp')), check_vma=False)
```

```python
import math
import jax
import jax.numpy as jnp
from jax import lax
from jax.experimental import pallas as pl
from jax.experimental.pallas import tpu as pltpu
from jax.sharding import PartitionSpec as P

MTP_WEIGHT = 0.3
EPS = 1e-6
BF = jnp.bfloat16
F32 = jnp.float32


def norm_only(acts):
    acts_f = acts.astype(F32)
    return acts_f * lax.rsqrt(jnp.mean(acts_f * acts_f, axis=-1, keepdims=True) + EPS)


def norm_bf16(acts):
    return norm_only(acts).astype(BF)


def gain_norm(acts, gain):
    return (norm_only(acts) * gain.astype(F32)).astype(BF)


def gelu_bf16(pre_act):
    return jax.nn.gelu(pre_act).astype(BF)


def dot(a, b, dims):
    return lax.dot_general(a, b, (dims, ((), ())), preferred_element_type=F32)


def normed_heads(hid, rows, gain_f, gain_h, gain_e, gain_m, w_proj, u_up, u_down):
    main = gain_norm(hid, gain_f)
    joined = jnp.concatenate([gain_norm(hid, gain_h), gain_norm(rows, gain_e)], axis=-1)
    state = jnp.dot(joined, w_proj, preferred_element_type=F32).astype(BF)
    inner = gelu_bf16(jnp.dot(gain_norm(state, gain_m), u_up, preferred_element_type=F32))
    state = (state.astype(F32) + jnp.dot(inner, u_down, preferred_element_type=F32)).astype(BF)
    return main, gain_norm(state, gain_f)


MESH = pl.DeviceIdType.MESH
VMEM_LIMIT = 64 * 1024 * 1024 - 65536
FF_STEP = 512
WG_STEP = 512
WG_ROWS = 512
TILE = 256
GELU_K = math.sqrt(2.0 / math.pi)


def gelu_slope(x):
    t = jnp.tanh(GELU_K * (x + 0.044715 * x * x * x))
    return 0.5 * (1.0 + t) + 0.5 * x * (1.0 - t * t) * (GELU_K * (1.0 + 3.0 * 0.044715 * x * x))


def greet(peers):
    barrier = pltpu.get_barrier_semaphore()
    for peer in peers:
        pl.semaphore_signal(barrier, inc=1, device_id=peer, device_id_type=MESH)
    pl.semaphore_wait(barrier, len(peers))


def pipe_fwd_kernel(n_stages, x_ref, wi_hbm, wo_hbm, in_ref, hid_ref, wi, wo, recv, send, hid_buf, acc, w_sem, send_sem, recv_sem, hsend_sem, hrecv_sem):
    stage = lax.axis_index('pp')
    data = lax.axis_index('dp')
    last = n_stages - 1
    chunk = send.shape[1]
    ffn = wi.shape[1]
    load_in = pltpu.make_async_copy(wi_hbm, wi, w_sem.at[0])
    load_out = pltpu.make_async_copy(wo_hbm, wo, w_sem.at[1])
    load_in.start()
    load_out.start()
    greet([(data, lax.rem(stage + k, n_stages)) for k in range(1, n_stages)])

    def onward(c):
        return pltpu.make_async_remote_copy(
            src_ref=send.at[c], dst_ref=recv.at[c], send_sem=send_sem.at[c], recv_sem=recv_sem.at[c],
            device_id=(data, lax.rem(stage + 1, n_stages)), device_id_type=MESH)

    def deliver(c):
        return pltpu.make_async_remote_copy(
            src_ref=send.at[c], dst_ref=hid_buf, send_sem=hsend_sem.at[c], recv_sem=hrecv_sem,
            device_id=(data, c), device_id_type=MESH)

    load_in.wait()
    load_out.wait()

    def step(c, carry):
        rows = pl.ds(pl.multiple_of(c * chunk, chunk), chunk)

        @pl.when(stage == 0)
        def _():
            in_ref[rows, :] = x_ref[rows, :]

        @pl.when(stage > 0)
        def _():
            onward(c).wait_recv()
            in_ref[rows, :] = recv[c]

        acts = in_ref[rows, :].astype(F32)
        normed = norm_only(acts).astype(BF)
        acc[...] = acts

        def ffn_step(t, inner):
            cols = pl.ds(pl.multiple_of(t * FF_STEP, FF_STEP), FF_STEP)
            pre = jnp.dot(normed, wi[:, cols], preferred_element_type=F32)
            acc[...] += jnp.dot(gelu_bf16(pre), wo[cols, :], preferred_element_type=F32)
            return inner

        lax.fori_loop(0, ffn // FF_STEP, ffn_step, 0)
        send[c] = acc[...].astype(BF)

        @pl.when(stage < last)
        def _():
            onward(c).start()

        @pl.when((stage == last) & (c < last))
        def _():
            deliver(c).start()

        return carry

    lax.fori_loop(0, n_stages, step, 0)

    @pl.when(stage < last)
    def _():
        for c in range(n_stages):
            onward(c).wait_send()
        deliver(0).wait_recv()
        hid_ref[...] = hid_buf[...]

    @pl.when(stage == last)
    def _():
        hid_ref[...] = send[last]
        for c in range(last):
            deliver(c).wait_send()


def pipe_fwd(x, w_in, w_out, n_stages):
    n_tok, hidden = x.shape
    ffn = w_in.shape[1]
    chunk = n_tok // n_stages
    vmem = pl.BlockSpec(memory_space=pltpu.VMEM)
    hbm = pl.BlockSpec(memory_space=pl.ANY)
    return pl.pallas_call(
        lambda *refs: pipe_fwd_kernel(n_stages, *refs),
        in_specs=[vmem, hbm, hbm],
        out_specs=[vmem, vmem],
        out_shape=[jax.ShapeDtypeStruct((n_tok, hidden), BF), jax.ShapeDtypeStruct((chunk, hidden), BF)],
        scratch_shapes=[
            pltpu.VMEM((hidden, ffn), BF),
            pltpu.VMEM((ffn, hidden), BF),
            pltpu.VMEM((n_stages, chunk, hidden), BF),
            pltpu.VMEM((n_stages, chunk, hidden), BF),
            pltpu.VMEM((chunk, hidden), BF),
            pltpu.VMEM((chunk, hidden), F32),
            pltpu.SemaphoreType.DMA((2,)),
            pltpu.SemaphoreType.DMA((n_stages,)),
            pltpu.SemaphoreType.DMA((n_stages,)),
            pltpu.SemaphoreType.DMA((n_stages,)),
            pltpu.SemaphoreType.DMA,
        ],
        compiler_params=pltpu.CompilerParams(collective_id=0, has_side_effects=True, vmem_limit_bytes=VMEM_LIMIT),
        cost_estimate=pl.CostEstimate(flops=4 * n_tok * hidden * ffn * 4, bytes_accessed=4 * hidden * ffn, transcendentals=0),
        name='pipe_fwd',
    )(x, w_in, w_out)


def pipe_bwd_kernel(n_stages, n_data, top_ref, acts_ref, wi_hbm, wo_hbm, dall_hbm, fall_hbm, wi, wo, slope, top, dall, fall, acc,
                    w_sem, csend, crecv, tsend, trecv, gsend, grecv, fsend, frecv, o_sem):
    stage = lax.axis_index('pp')
    data = lax.axis_index('dp')
    last = n_stages - 1
    chunk = top.shape[1]
    ffn = wi.shape[1]
    load_in = pltpu.make_async_copy(wi_hbm, wi, w_sem.at[0])
    load_out = pltpu.make_async_copy(wo_hbm, wo, w_sem.at[1])
    load_in.start()
    load_out.start()
    greet([(data, lax.rem(stage + k, n_stages)) for k in range(1, n_stages)]
          + [(lax.rem(data + k, n_data), stage) for k in range(1, n_data)])

    def hand_in(slot):
        return pltpu.make_async_remote_copy(
            src_ref=top_ref, dst_ref=top.at[slot], send_sem=tsend, recv_sem=trecv.at[slot],
            device_id=(data, last), device_id_type=MESH)

    def back(c):
        return pltpu.make_async_remote_copy(
            src_ref=fall.at[data, c], dst_ref=dall.at[data, c], send_sem=csend.at[c], recv_sem=crecv.at[c],
            device_id=(data, lax.rem(stage + last, n_stages)), device_id_type=MESH)

    def share(buf, owner, k, c, send_sem, recv_sem):
        return pltpu.make_async_remote_copy(
            src_ref=buf.at[owner, c], dst_ref=buf.at[owner, c], send_sem=send_sem.at[k - 1, c], recv_sem=recv_sem.at[k - 1, c],
            device_id=(lax.rem(data + k, n_data), stage), device_id_type=MESH)

    @pl.when(stage < last)
    def _():
        hand_in(stage).start()

    @pl.when(stage == last)
    def _():
        top[last] = top_ref[...]

    load_in.wait()
    normed_all = norm_only(acts_ref[...].astype(F32)).astype(BF)

    def slope_step(t, carry):
        cols = pl.ds(pl.multiple_of(t * FF_STEP, FF_STEP), FF_STEP)
        slope[:, cols] = gelu_slope(jnp.dot(normed_all, wi[:, cols], preferred_element_type=F32))
        return carry

    lax.fori_loop(0, ffn // FF_STEP, slope_step, 0)
    load_out.wait()

    def step(c, carry):
        rows = pl.ds(pl.multiple_of(c * chunk, chunk), chunk)

        @pl.when((stage == last) & (c < last))
        def _():
            hand_in(c).wait_recv()

        @pl.when(stage == last)
        def _():
            dall[data, c] = top[c]

        @pl.when(stage < last)
        def _():
            back(c).wait_recv()

        d_out = dall[data, c]
        acc[...] = jnp.zeros_like(acc)

        def ffn_step(t, inner):
            cols = pl.ds(pl.multiple_of(t * FF_STEP, FF_STEP), FF_STEP)
            d_act = dot(d_out, wo[cols, :], ((1,), (1,))).astype(BF).astype(F32)
            d_pre = (d_act * slope[rows, cols]).astype(BF)
            acc[...] += dot(d_pre, wi[:, cols], ((1,), (1,)))
            return inner

        lax.fori_loop(0, ffn // FF_STEP, ffn_step, 0)
        d_norm = acc[...].astype(BF).astype(F32)
        acts = acts_ref[rows, :].astype(F32)
        scale = lax.rsqrt(jnp.mean(acts * acts, axis=-1, keepdims=True) + EPS)
        inner_mean = jnp.mean(d_norm * acts, axis=-1, keepdims=True)
        d_acts = (d_norm * scale - acts * (scale * scale * scale * inner_mean)).astype(BF)
        fall[data, c] = (d_out.astype(F32) + d_acts.astype(F32)).astype(BF)

        @pl.when(stage > 0)
        def _():
            back(c).start()

        for k in range(1, n_data):
            share(dall, data, k, c, gsend, grecv).start()

        @pl.when(stage == 0)
        def _():
            for k in range(1, n_data):
                share(fall, data, k, c, fsend, frecv).start()

        return carry

    lax.fori_loop(0, n_stages, step, 0)

    @pl.when(stage < last)
    def _():
        hand_in(stage).wait_send()

    @pl.when(stage > 0)
    def _():
        for c in range(n_stages):
            back(c).wait_send()

    for k in range(1, n_data):
        for c in range(n_stages):
            share(dall, data, k, c, gsend, grecv).wait_send()
            share(dall, lax.rem(data + n_data - k, n_data), k, c, gsend, grecv).wait_recv()
    save = pltpu.make_async_copy(dall, dall_hbm, o_sem.at[0])
    save.start()

    @pl.when(stage == 0)
    def _():
        for k in range(1, n_data):
            for c in range(n_stages):
                share(fall, data, k, c, fsend, frecv).wait_send()
                share(fall, lax.rem(data + n_data - k, n_data), k, c, fsend, frecv).wait_recv()
        save_first = pltpu.make_async_copy(fall, fall_hbm, o_sem.at[1])
        save_first.start()
        save_first.wait()

    save.wait()


def pipe_bwd(d_top, acts, w_in, w_out, n_stages, n_data):
    n_tok, hidden = acts.shape
    ffn = w_in.shape[1]
    chunk = n_tok // n_stages
    vmem = pl.BlockSpec(memory_space=pltpu.VMEM)
    hbm = pl.BlockSpec(memory_space=pl.ANY)
    full = (n_data, n_stages, chunk, hidden)
    dma = pltpu.SemaphoreType.DMA
    return pl.pallas_call(
        lambda *refs: pipe_bwd_kernel(n_stages, n_data, *refs),
        in_specs=[vmem, vmem, hbm, hbm],
        out_specs=[hbm, hbm],
        out_shape=[jax.ShapeDtypeStruct(full, BF), jax.ShapeDtypeStruct(full, BF)],
        scratch_shapes=[
            pltpu.VMEM((hidden, ffn), BF),
            pltpu.VMEM((ffn, hidden), BF),
            pltpu.VMEM((n_tok, ffn), F32),
            pltpu.VMEM((n_stages, chunk, hidden), BF),
            pltpu.VMEM(full, BF),
            pltpu.VMEM(full, BF),
            pltpu.VMEM((chunk, hidden), F32),
            dma((2,)), dma((n_stages,)), dma((n_stages,)), dma, dma((n_stages,)),
            dma((n_data - 1, n_stages)), dma((n_data - 1, n_stages)),
            dma((n_data - 1, n_stages)), dma((n_data - 1, n_stages)), dma((2,)),
        ],
        compiler_params=pltpu.CompilerParams(collective_id=1, has_side_effects=True, vmem_limit_bytes=VMEM_LIMIT),
        cost_estimate=pl.CostEstimate(flops=6 * n_tok * hidden * ffn * 4, bytes_accessed=4 * hidden * ffn, transcendentals=0),
        name='pipe_bwd',
    )(d_top, acts, w_in, w_out)


def wgrad_kernel(n_ref, nt_ref, d_ref, wi_ref, wo_ref, gi_ref, go_ref):
    gi_ref[...] = jnp.zeros_like(gi_ref)
    go_ref[...] = jnp.zeros_like(go_ref)
    for b in range(n_ref.shape[0] // WG_ROWS):
        rows = slice(b * WG_ROWS, (b + 1) * WG_ROWS)
        pre = jnp.dot(n_ref[rows, :], wi_ref[...], preferred_element_type=F32)
        d_act = dot(d_ref[rows, :], wo_ref[...], ((1,), (1,))).astype(BF).astype(F32)
        t = jnp.tanh(GELU_K * (pre + 0.044715 * pre * pre * pre))
        half = 0.5 * (1.0 + t)
        act = (pre * half).astype(BF)
        slope = half + 0.5 * pre * (1.0 - t * t) * (GELU_K * (1.0 + 3.0 * 0.044715 * pre * pre))
        gi_ref[...] += jnp.dot(nt_ref[:, rows], (d_act * slope).astype(BF), preferred_element_type=F32)
        go_ref[...] += dot(act, d_ref[rows, :], ((0,), (0,)))


def stage_wgrad(normed, normed_t, w_in, w_out, d_out):
    n_all, hidden = normed.shape
    ffn = w_in.shape[1]
    vmem = pl.BlockSpec(memory_space=pltpu.VMEM)
    cols = pl.BlockSpec((hidden, WG_STEP), lambda i: (0, i))
    rows = pl.BlockSpec((WG_STEP, hidden), lambda i: (i, 0))
    return pl.pallas_call(
        wgrad_kernel,
        grid=(ffn // WG_STEP,),
        in_specs=[vmem, vmem, vmem, cols, rows],
        out_specs=[cols, rows],
        out_shape=[jax.ShapeDtypeStruct((hidden, ffn), F32), jax.ShapeDtypeStruct((ffn, hidden), F32)],
        compiler_params=pltpu.CompilerParams(vmem_limit_bytes=VMEM_LIMIT),
        cost_estimate=pl.CostEstimate(flops=8 * n_all * hidden * ffn, bytes_accessed=12 * hidden * ffn, transcendentals=n_all * ffn),
        name='stage_wgrad',
    )(normed, normed_t, d_out, w_in, w_out)


def scatter_kernel(scale, firsts, starts_ref, rows_ref, perm_ref, *refs):
    pieces = refs[:-4]
    first_ref, next_ref, out_ref, upd = refs[-4:]
    tile = pl.program_id(0)
    n_tiles = pl.num_programs(0)
    owner = starts_ref[n_tiles + 1] == 1
    n_first = first_ref.shape[0]

    @pl.when(owner & (tile == 0))
    def _():
        upd[0:n_first] = first_ref[...].astype(F32) * scale
        upd[n_first:] = next_ref[...].astype(F32) * scale

    @pl.when(jnp.logical_not(owner))
    def _():
        out_ref[...] = jnp.zeros_like(out_ref)

    for q, piece in enumerate(pieces):
        @pl.when(owner & (tile >= firsts[q]) & (tile < firsts[q + 1]))
        def _():
            out_ref[...] = piece[...]

    def add_row(k, carry):
        row = rows_ref[k] - tile * TILE
        out_ref[pl.ds(row, 1), :] += upd[pl.ds(perm_ref[k], 1), :]
        return carry

    lax.fori_loop(starts_ref[tile], starts_ref[tile + 1], add_row, 0)


def scatter_plan(ids, owner, n_rows):
    n_tiles = pl.cdiv(n_rows, TILE)
    sorted_ids, perm = lax.sort((ids, lax.iota(jnp.int32, ids.shape[0])), num_keys=1)
    bounds = jnp.minimum(jnp.arange(n_tiles + 1, dtype=jnp.int32) * TILE, n_rows)
    starts = jnp.sum((ids[None, :] < bounds[:, None]).astype(jnp.int32), axis=1)
    return jnp.concatenate([starts, owner.astype(jnp.int32)[None]]), sorted_ids, perm


def scatter_rows(pieces, n_rows, first, following, plan, scale):
    hidden = first.shape[1]
    n_tiles = pl.cdiv(n_rows, TILE)
    n_upd = plan[1].shape[0]
    firsts = [0]
    for piece in pieces:
        firsts.append(firsts[-1] + piece.shape[0] // TILE)

    def piece_map(q):
        return lambda i, starts_ref, *_: (jnp.clip(i - firsts[q], 0, firsts[q + 1] - firsts[q] - 1) * starts_ref[n_tiles + 1], 0)

    vmem = pl.BlockSpec(memory_space=pltpu.VMEM)
    return pl.pallas_call(
        lambda *refs: scatter_kernel(scale, firsts, *refs),
        grid_spec=pltpu.PrefetchScalarGridSpec(
            num_scalar_prefetch=3,
            grid=(n_tiles,),
            in_specs=[pl.BlockSpec((TILE, hidden), piece_map(q)) for q in range(len(pieces))] + [vmem, vmem],
            out_specs=pl.BlockSpec((TILE, hidden), lambda i, *_: (i, 0)),
            scratch_shapes=[pltpu.VMEM((n_upd, hidden), F32)],
        ),
        out_shape=jax.ShapeDtypeStruct((n_rows, hidden), F32),
        compiler_params=pltpu.CompilerParams(vmem_limit_bytes=VMEM_LIMIT),
        name='scatter_rows',
    )(*plan, *pieces, first, following)


VTILE = 512
SHARES = (6, 6, 2, 2)
ROWS = 512
LOWEST = float(jnp.finfo(jnp.float32).min)


def head_fwd_kernel(meta, n_ref, e_ref, z_ref, top_ref, sum_ref):
    tile = pl.program_id(0)

    @pl.when(tile == 0)
    def _():
        top_ref[...] = jnp.full_like(top_ref, LOWEST)
        sum_ref[...] = jnp.zeros_like(sum_ref)

    @pl.when(tile < meta[0])
    def _():
        keep = tile * VTILE + lax.broadcasted_iota(jnp.int32, (ROWS, VTILE), 1) < meta[1]

        def block(b, carry):
            rows = pl.ds(pl.multiple_of(b * ROWS, ROWS), ROWS)
            z = dot(n_ref[rows, :], e_ref[...], ((1,), (1,)))
            z = jnp.where(keep, z, LOWEST)
            z_ref[rows, :] = z
            lanes = [z[:, k * 128:(k + 1) * 128] for k in range(VTILE // 128)]
            old = top_ref[rows, :]
            new = old
            for part in lanes:
                new = jnp.maximum(new, part)
            total = sum_ref[rows, :] * jnp.exp(old - new)
            for part in lanes:
                total = total + jnp.exp(part - new)
            top_ref[rows, :] = new
            sum_ref[rows, :] = total
            return carry

        lax.fori_loop(0, n_ref.shape[0] // ROWS, block, 0, unroll=True)


def head_fwd(meta, norm_all, table_q):
    n_all, hidden = norm_all.shape
    tiles = table_q.shape[0] // VTILE
    vmem = pl.BlockSpec(memory_space=pltpu.VMEM)
    return pl.pallas_call(
        head_fwd_kernel,
        grid_spec=pltpu.PrefetchScalarGridSpec(
            num_scalar_prefetch=1,
            grid=(tiles,),
            in_specs=[vmem, pl.BlockSpec((VTILE, hidden), lambda i, meta: (jnp.minimum(i, meta[0] - 1), 0))],
            out_specs=[pl.BlockSpec((n_all, VTILE), lambda i, meta: (0, jnp.minimum(i, meta[0] - 1))), vmem, vmem],
        ),
        out_shape=[jax.ShapeDtypeStruct((n_all, tiles * VTILE), F32)] + [jax.ShapeDtypeStruct((n_all, 128), F32)] * 2,
        compiler_params=pltpu.CompilerParams(vmem_limit_bytes=VMEM_LIMIT),
        cost_estimate=pl.CostEstimate(flops=2 * n_all * hidden * tiles * VTILE, bytes_accessed=4 * n_all * tiles * VTILE, transcendentals=n_all * tiles * VTILE),
        name='head_fwd',
    )(meta, norm_all, table_q)


def head_bwd_kernel(weight, meta, n_ref, e_ref, z_ref, lse_ref, tgt_ref, *refs):
    prev_ref = refs[0] if len(refs) == 4 else None
    dn_ref, de_ref, grad = refs[-3:]
    tile = pl.program_id(0)

    @pl.when(tile == 0)
    def _():
        dn_ref[...] = jnp.zeros_like(dn_ref)

    @pl.when(tile < meta[0])
    def _():
        column = tile * VTILE + lax.broadcasted_iota(jnp.int32, (ROWS, VTILE), 1)

        def block(b, carry):
            rows = pl.ds(pl.multiple_of(b * ROWS, ROWS), ROWS)
            prob = jnp.exp(z_ref[rows, :] - lse_ref[rows, :])
            hit = column == tgt_ref[rows, :]
            g = (jnp.where(hit, prob - 1.0, prob) * weight).astype(BF)
            grad[rows, :] = g
            dn_ref[rows, :] += jnp.dot(g, e_ref[...], preferred_element_type=F32)
            return carry

        lax.fori_loop(0, n_ref.shape[0] // ROWS, block, 0, unroll=True)
        de = dot(grad[...], n_ref[...], ((0,), (0,)))
        de_ref[...] = de if prev_ref is None else de + prev_ref[...]


def head_bwd(meta, norm_all, table_q, z, lse, targets, weight, prev):
    n_all, hidden = norm_all.shape
    tiles = table_q.shape[0] // VTILE
    vmem = pl.BlockSpec(memory_space=pltpu.VMEM)
    vrows = pl.BlockSpec((VTILE, hidden), lambda i, meta: (jnp.minimum(i, meta[0] - 1), 0))
    vcols = pl.BlockSpec((n_all, VTILE), lambda i, meta: (0, jnp.minimum(i, meta[0] - 1)))
    extra = [] if prev is None else [prev]
    return pl.pallas_call(
        lambda *refs: head_bwd_kernel(weight, *refs),
        grid_spec=pltpu.PrefetchScalarGridSpec(
            num_scalar_prefetch=1,
            grid=(tiles,),
            in_specs=[vmem, vrows, vcols, vmem, vmem] + [vrows] * len(extra),
            out_specs=[vmem, vrows],
            scratch_shapes=[pltpu.VMEM((n_all, VTILE), BF)],
        ),
        out_shape=[jax.ShapeDtypeStruct((n_all, hidden), F32), jax.ShapeDtypeStruct(table_q.shape, F32)],
        compiler_params=pltpu.CompilerParams(vmem_limit_bytes=VMEM_LIMIT),
        cost_estimate=pl.CostEstimate(flops=4 * n_all * hidden * tiles * VTILE, bytes_accessed=4 * n_all * tiles * VTILE, transcendentals=n_all * tiles * VTILE),
        name='head_bwd',
    )(meta, norm_all, table_q, z, lse[:, None], targets[:, None], *extra)


def solution(mesh):
    n_stages = mesh.shape['pp']
    n_data = mesh.shape['dp']
    both = ('dp', 'pp')

    firsts = [VTILE * sum(SHARES[:q]) for q in range(n_stages + 1)]

    def from_first(pieces, stage):
        mine = jnp.where(stage == 0, pieces[0], jnp.zeros_like(pieces[0]))
        for q in range(1, n_stages):
            mine = mine + lax.ppermute(pieces[q], 'pp', [(0, q)])
        return mine

    def device_body(tokens, emb_s, w_up, w_down, gain_f, gain_h, gain_e, gain_m, w_proj, u_up, u_down):
        stage = lax.axis_index('pp')
        data = lax.axis_index('dp')
        is_first = stage == 0
        n_micro, rows_dev, width = tokens.shape
        seq_len = width - 2
        table = emb_s[0]
        v_own, hidden = table.shape
        v_dev = VTILE * max(SHARES)
        emb_scale = math.sqrt(hidden)
        w_in = w_up[0, 0]
        w_out = w_down[0, 0]
        n_seq = n_micro * rows_dev
        n_own = n_seq * seq_len
        n_all = n_own * n_data
        loss_scale = 1.0 / n_all
        q_seq = n_seq // n_stages
        n_q = q_seq * seq_len
        n_pos = n_seq * width

        tok_all = lax.all_gather(tokens.reshape(n_seq, width), 'dp', axis=0, tiled=True)
        local_ids = tok_all.reshape(-1) - data * v_own
        owned = (local_ids >= 0) & (local_ids < v_own)
        got = jnp.take(table, jnp.clip(local_ids, 0, v_own - 1), axis=0)
        got = jnp.where(owned[:, None], got, 0.0).astype(BF).reshape(n_data, n_pos, hidden)
        rows = lax.dynamic_index_in_dim(got, data, 0, keepdims=False)
        for k in range(1, n_data):
            outgoing = lax.dynamic_index_in_dim(got, lax.rem(data + k, n_data), 0, keepdims=False)
            pairs = [(d * n_stages, ((d + k) % n_data) * n_stages) for d in range(n_data)]
            rows = rows + lax.ppermute(outgoing, both, pairs)
        rows = rows.reshape(n_seq, width, hidden)

        def piece(q):
            part = table[firsts[q]:min(firsts[q + 1], v_own)].astype(BF)
            return jnp.pad(part, ((0, VTILE * SHARES[q] - part.shape[0]), (0, 0)))

        table_q = jnp.where(is_first, piece(0), 0)
        for q in range(1, n_stages):
            sent = lax.ppermute(piece(q), 'pp', [(0, q)])
            table_q = table_q + jnp.pad(sent, ((0, v_dev - sent.shape[0]), (0, 0)))
        rows_q = from_first([rows[q * q_seq:(q + 1) * q_seq] for q in range(n_stages)], stage)

        first_in = (rows[:, 0:seq_len].astype(F32) * emb_scale).astype(BF).reshape(n_own, hidden)
        stage_in, hid_q = pipe_fwd(first_in, w_in, w_out, n_stages)
        mtp_rows = (rows_q[:, 1:seq_len + 1].astype(F32) * emb_scale).astype(BF).reshape(n_q, hidden)

        def heads(hid, mtp):
            return normed_heads(hid, mtp, gain_f, gain_h, gain_e, gain_m, w_proj, u_up, u_down)

        (main_q, next_q), heads_back = jax.vjp(heads, hid_q, mtp_rows)

        dev_index = data * n_stages + stage
        shard_first = jnp.asarray(firsts[:-1], jnp.int32)[stage]
        shard_last = jnp.minimum(jnp.asarray(firsts[1:], jnp.int32)[stage], v_own)
        valid = shard_last - shard_first
        meta = jnp.stack([jnp.asarray(SHARES, jnp.int32)[stage], valid])

        def targets_of(ids):
            local = ids - data_base
            return jnp.where((local >= 0) & (local < valid), local, -1)

        data_base = data * v_own + shard_first

        def collect(partial):
            return lax.psum_scatter(partial, both, scatter_dimension=0, tiled=True).astype(BF)

        mid_all = tok_all[:, 1:seq_len + 1].reshape(n_all)
        out_all = tok_all[:, 2:seq_len + 2].reshape(n_all)
        main_all = lax.all_gather(main_q, both, axis=0, tiled=True)
        next_all = lax.all_gather(next_q, both, axis=0, tiled=True)
        stage_in_late, main_all, next_all = lax.optimization_barrier((stage_in, main_all, next_all))
        acts_all = lax.all_gather(stage_in_late, 'dp', axis=0, tiled=True)
        main_z, main_top, main_sum = head_fwd(meta, main_all, table_q)
        next_z, next_top, next_sum = head_fwd(meta, next_all, table_q)
        lane_top = jnp.stack([main_top, next_top])
        top = jnp.max(lane_top, axis=-1)
        total = jnp.sum(jnp.stack([main_sum, next_sum]) * jnp.exp(lane_top - top[..., None]), axis=-1)
        stats = lax.all_gather(jnp.stack([top, total]), both, axis=0)
        top_all = jnp.max(stats[:, 0], axis=0)
        sum_all = jnp.sum(stats[:, 1] * jnp.exp(stats[:, 0] - top_all[None]), axis=0)
        main_lse, next_lse = jnp.log(sum_all) + top_all
        next_part, next_g = head_bwd(meta, next_all, table_q, next_z, next_lse, targets_of(out_all), MTP_WEIGHT * loss_scale, None)
        d_next = collect(next_part)
        main_part, g_table = head_bwd(meta, main_all, table_q, main_z, main_lse, targets_of(mid_all), loss_scale, next_g)
        d_main = collect(main_part)

        def own(lse):
            return lax.dynamic_slice(lse, (dev_index * n_q,), (n_q,))

        mid_rows = rows_q[:, 1:seq_len + 1].reshape(n_q, hidden).astype(F32)
        out_rows = rows_q[:, 2:seq_len + 2].reshape(n_q, hidden).astype(F32)
        main_pick = jnp.sum(main_q.astype(F32) * mid_rows, axis=-1)
        next_pick = jnp.sum(next_q.astype(F32) * out_rows, axis=-1)
        local_loss = (jnp.sum(own(main_lse) - main_pick) + MTP_WEIGHT * jnp.sum(own(next_lse) - next_pick)) * loss_scale

        d_hid_q, d_rows_q = heads_back((d_main, d_next))
        d_rows_all = lax.all_gather(d_rows_q, both, axis=0, tiled=True)

        look_ids = jnp.concatenate([tok_all[:, 0:seq_len].reshape(-1), mid_all]) - data * v_own
        look_ids = jnp.where(is_first & (look_ids >= 0) & (look_ids < v_own), look_ids, v_own)
        plan = scatter_plan(look_ids, is_first, v_own)
        normed = norm_bf16(acts_all)
        prepared = lax.optimization_barrier((d_hid_q, normed, normed.T, plan))
        d_hid_q, normed, normed_t, plan = prepared
        d_out_all, d_first_all = pipe_bwd(d_hid_q, stage_in, w_in, w_out, n_stages, n_data)
        g_late, d_out_all, d_first_all = lax.optimization_barrier((g_table, d_out_all, d_first_all))
        pieces = [g_table] + [lax.ppermute(g_late[0:VTILE * SHARES[q]], 'pp', [(q, 0)]) for q in range(1, n_stages)]
        d_out_all = d_out_all.reshape(n_all, hidden)
        d_first_all = d_first_all.reshape(n_all, hidden)
        g_in, g_out = stage_wgrad(normed, normed_t, w_in, w_out, d_out_all)

        d_first_all, g_in = lax.optimization_barrier((d_first_all, g_in))
        g_shard = scatter_rows(pieces, v_own, d_first_all, d_rows_all, plan, emb_scale)
        local_loss, _ = lax.optimization_barrier((local_loss, g_shard))
        loss = lax.psum(local_loss, both)
        return loss, g_shard[None], g_in[None, None], g_out[None, None]

    return jax.shard_map(device_body, mesh=mesh, in_specs=(P(None, 'dp', None), P('pp', 'dp', None), P('pp'), P('pp'), P(), P(), P(), P(), P(), P(), P()), out_specs=(P(), P('pp', 'dp', None), P('pp'), P('pp')), check_vma=False)
```

```python
import math
import jax
import jax.numpy as jnp
from jax import lax
from jax.experimental import pallas as pl
from jax.experimental.pallas import tpu as pltpu
from jax.sharding import PartitionSpec as P

MTP_WEIGHT = 0.3
EPS = 1e-6
BF = jnp.bfloat16
F32 = jnp.float32


def norm_only(acts):
    acts_f = acts.astype(F32)
    return acts_f * lax.rsqrt(jnp.mean(acts_f * acts_f, axis=-1, keepdims=True) + EPS)


def norm_bf16(acts):
    return norm_only(acts).astype(BF)


def gain_norm(acts, gain):
    return (norm_only(acts) * gain.astype(F32)).astype(BF)


def gelu_bf16(pre_act):
    return jax.nn.gelu(pre_act).astype(BF)


def dot(a, b, dims):
    return lax.dot_general(a, b, (dims, ((), ())), preferred_element_type=F32)


def normed_heads(hid, rows, gain_f, gain_h, gain_e, gain_m, w_proj, u_up, u_down):
    main = gain_norm(hid, gain_f)
    joined = jnp.concatenate([gain_norm(hid, gain_h), gain_norm(rows, gain_e)], axis=-1)
    state = jnp.dot(joined, w_proj, preferred_element_type=F32).astype(BF)
    inner = gelu_bf16(jnp.dot(gain_norm(state, gain_m), u_up, preferred_element_type=F32))
    state = (state.astype(F32) + jnp.dot(inner, u_down, preferred_element_type=F32)).astype(BF)
    return main, gain_norm(state, gain_f)


MESH = pl.DeviceIdType.MESH
VMEM_LIMIT = 64 * 1024 * 1024 - 65536
FF_STEP = 2048
WG_STEP = 512
WG_ROWS = 512
TILE = 256
GELU_K = math.sqrt(2.0 / math.pi)


def gelu_slope(x):
    t = jnp.tanh(GELU_K * (x + 0.044715 * x * x * x))
    return 0.5 * (1.0 + t) + 0.5 * x * (1.0 - t * t) * (GELU_K * (1.0 + 3.0 * 0.044715 * x * x))


def greet(peers):
    barrier = pltpu.get_barrier_semaphore()
    for peer in peers:
        pl.semaphore_signal(barrier, inc=1, device_id=peer, device_id_type=MESH)
    pl.semaphore_wait(barrier, len(peers))


def pipe_fwd_kernel(n_stages, x_ref, wi_hbm, wo_hbm, in_ref, hid_ref, wi, wo, recv, send, hid_buf, acc, w_sem, send_sem, recv_sem, hsend_sem, hrecv_sem):
    stage = lax.axis_index('pp')
    data = lax.axis_index('dp')
    last = n_stages - 1
    chunk = send.shape[1]
    ffn = wi.shape[1]
    load_in = pltpu.make_async_copy(wi_hbm, wi, w_sem.at[0])
    load_out = pltpu.make_async_copy(wo_hbm, wo, w_sem.at[1])
    load_in.start()
    load_out.start()
    greet([(data, lax.rem(stage + k, n_stages)) for k in range(1, n_stages)])

    def onward(c):
        return pltpu.make_async_remote_copy(
            src_ref=send.at[c], dst_ref=recv.at[c], send_sem=send_sem.at[c], recv_sem=recv_sem.at[c],
            device_id=(data, lax.rem(stage + 1, n_stages)), device_id_type=MESH)

    def deliver(c):
        return pltpu.make_async_remote_copy(
            src_ref=send.at[c], dst_ref=hid_buf, send_sem=hsend_sem.at[c], recv_sem=hrecv_sem,
            device_id=(data, c), device_id_type=MESH)

    load_in.wait()
    load_out.wait()

    def step(c, carry):
        rows = pl.ds(pl.multiple_of(c * chunk, chunk), chunk)

        @pl.when(stage == 0)
        def _():
            in_ref[rows, :] = x_ref[rows, :]

        @pl.when(stage > 0)
        def _():
            onward(c).wait_recv()
            in_ref[rows, :] = recv[c]

        acts = in_ref[rows, :].astype(F32)
        normed = norm_only(acts).astype(BF)
        acc[...] = acts

        def ffn_step(t, inner):
            cols = pl.ds(pl.multiple_of(t * FF_STEP, FF_STEP), FF_STEP)
            pre = jnp.dot(normed, wi[:, cols], preferred_element_type=F32)
            acc[...] += jnp.dot(gelu_bf16(pre), wo[cols, :], preferred_element_type=F32)
            return inner

        lax.fori_loop(0, ffn // FF_STEP, ffn_step, 0)
        send[c] = acc[...].astype(BF)

        @pl.when(stage < last)
        def _():
            onward(c).start()

        @pl.when((stage == last) & (c < last))
        def _():
            deliver(c).start()

        return carry

    lax.fori_loop(0, n_stages, step, 0)

    @pl.when(stage < last)
    def _():
        for c in range(n_stages):
            onward(c).wait_send()
        deliver(0).wait_recv()
        hid_ref[...] = hid_buf[...]

    @pl.when(stage == last)
    def _():
        hid_ref[...] = send[last]
        for c in range(last):
            deliver(c).wait_send()


def pipe_fwd(x, w_in, w_out, n_stages):
    n_tok, hidden = x.shape
    ffn = w_in.shape[1]
    chunk = n_tok // n_stages
    vmem = pl.BlockSpec(memory_space=pltpu.VMEM)
    hbm = pl.BlockSpec(memory_space=pl.ANY)
    return pl.pallas_call(
        lambda *refs: pipe_fwd_kernel(n_stages, *refs),
        in_specs=[vmem, hbm, hbm],
        out_specs=[vmem, vmem],
        out_shape=[jax.ShapeDtypeStruct((n_tok, hidden), BF), jax.ShapeDtypeStruct((chunk, hidden), BF)],
        scratch_shapes=[
            pltpu.VMEM((hidden, ffn), BF),
            pltpu.VMEM((ffn, hidden), BF),
            pltpu.VMEM((n_stages, chunk, hidden), BF),
            pltpu.VMEM((n_stages, chunk, hidden), BF),
            pltpu.VMEM((chunk, hidden), BF),
            pltpu.VMEM((chunk, hidden), F32),
            pltpu.SemaphoreType.DMA((2,)),
            pltpu.SemaphoreType.DMA((n_stages,)),
            pltpu.SemaphoreType.DMA((n_stages,)),
            pltpu.SemaphoreType.DMA((n_stages,)),
            pltpu.SemaphoreType.DMA,
        ],
        compiler_params=pltpu.CompilerParams(collective_id=0, has_side_effects=True, vmem_limit_bytes=VMEM_LIMIT),
        cost_estimate=pl.CostEstimate(flops=4 * n_tok * hidden * ffn * 4, bytes_accessed=4 * hidden * ffn, transcendentals=0),
        name='pipe_fwd',
    )(x, w_in, w_out)


def pipe_bwd_kernel(n_stages, n_data, top_ref, acts_ref, wi_hbm, wo_hbm, dall_hbm, fall_hbm, wi, wo, slope, top, dall, fall, acc,
                    w_sem, csend, crecv, tsend, trecv, gsend, grecv, o_sem):
    stage = lax.axis_index('pp')
    data = lax.axis_index('dp')
    last = n_stages - 1
    chunk = top.shape[1]
    ffn = wi.shape[1]
    load_in = pltpu.make_async_copy(wi_hbm, wi, w_sem.at[0])
    load_out = pltpu.make_async_copy(wo_hbm, wo, w_sem.at[1])
    load_in.start()
    load_out.start()
    greet([(data, lax.rem(stage + k, n_stages)) for k in range(1, n_stages)]
          + [(lax.rem(data + k, n_data), stage) for k in range(1, n_data)])

    def hand_in(slot):
        return pltpu.make_async_remote_copy(
            src_ref=top_ref, dst_ref=top.at[slot], send_sem=tsend, recv_sem=trecv.at[slot],
            device_id=(data, last), device_id_type=MESH)

    def back(c):
        return pltpu.make_async_remote_copy(
            src_ref=fall.at[c], dst_ref=dall.at[data, c], send_sem=csend.at[c], recv_sem=crecv.at[c],
            device_id=(data, lax.rem(stage + last, n_stages)), device_id_type=MESH)

    def share(buf, owner, k, c, send_sem, recv_sem):
        return pltpu.make_async_remote_copy(
            src_ref=buf.at[owner, c], dst_ref=buf.at[owner, c], send_sem=send_sem.at[k - 1, c], recv_sem=recv_sem.at[k - 1, c],
            device_id=(lax.rem(data + k, n_data), stage), device_id_type=MESH)

    @pl.when(stage < last)
    def _():
        hand_in(stage).start()

    @pl.when(stage == last)
    def _():
        top[last] = top_ref[...]

    load_in.wait()
    normed_all = norm_only(acts_ref[...].astype(F32)).astype(BF)

    def slope_step(t, carry):
        cols = pl.ds(pl.multiple_of(t * FF_STEP, FF_STEP), FF_STEP)
        slope[:, cols] = gelu_slope(jnp.dot(normed_all, wi[:, cols], preferred_element_type=F32))
        return carry

    lax.fori_loop(0, ffn // FF_STEP, slope_step, 0)
    load_out.wait()

    def step(c, carry):
        rows = pl.ds(pl.multiple_of(c * chunk, chunk), chunk)

        @pl.when((stage == last) & (c < last))
        def _():
            hand_in(c).wait_recv()

        @pl.when(stage == last)
        def _():
            dall[data, c] = top[c]

        @pl.when(stage < last)
        def _():
            back(c).wait_recv()

        d_out = dall[data, c]
        acc[...] = jnp.zeros_like(acc)

        def ffn_step(t, inner):
            cols = pl.ds(pl.multiple_of(t * FF_STEP, FF_STEP), FF_STEP)
            d_act = dot(d_out, wo[cols, :], ((1,), (1,))).astype(BF).astype(F32)
            d_pre = (d_act * slope[rows, cols]).astype(BF)
            acc[...] += dot(d_pre, wi[:, cols], ((1,), (1,)))
            return inner

        lax.fori_loop(0, ffn // FF_STEP, ffn_step, 0)
        d_norm = acc[...].astype(BF).astype(F32)
        acts = acts_ref[rows, :].astype(F32)
        scale = lax.rsqrt(jnp.mean(acts * acts, axis=-1, keepdims=True) + EPS)
        inner_mean = jnp.mean(d_norm * acts, axis=-1, keepdims=True)
        d_acts = (d_norm * scale - acts * (scale * scale * scale * inner_mean)).astype(BF)
        fall[c] = (d_out.astype(F32) + d_acts.astype(F32)).astype(BF)

        @pl.when(stage > 0)
        def _():
            back(c).start()

        for k in range(1, n_data):
            share(dall, data, k, c, gsend, grecv).start()

        return carry

    lax.fori_loop(0, n_stages, step, 0)

    @pl.when(stage < last)
    def _():
        hand_in(stage).wait_send()

    @pl.when(stage > 0)
    def _():
        for c in range(n_stages):
            back(c).wait_send()

    for k in range(1, n_data):
        for c in range(n_stages):
            share(dall, data, k, c, gsend, grecv).wait_send()
            share(dall, lax.rem(data + n_data - k, n_data), k, c, gsend, grecv).wait_recv()
    save = pltpu.make_async_copy(dall, dall_hbm, o_sem.at[0])
    save.start()

    save_first = pltpu.make_async_copy(fall, fall_hbm, o_sem.at[1])
    save_first.start()
    save_first.wait()
    save.wait()


def pipe_bwd(d_top, acts, w_in, w_out, n_stages, n_data):
    n_tok, hidden = acts.shape
    ffn = w_in.shape[1]
    chunk = n_tok // n_stages
    vmem = pl.BlockSpec(memory_space=pltpu.VMEM)
    hbm = pl.BlockSpec(memory_space=pl.ANY)
    full = (n_data, n_stages, chunk, hidden)
    dma = pltpu.SemaphoreType.DMA
    return pl.pallas_call(
        lambda *refs: pipe_bwd_kernel(n_stages, n_data, *refs),
        in_specs=[vmem, vmem, hbm, hbm],
        out_specs=[hbm, hbm],
        out_shape=[jax.ShapeDtypeStruct(full, BF), jax.ShapeDtypeStruct(full[1:], BF)],
        scratch_shapes=[
            pltpu.VMEM((hidden, ffn), BF),
            pltpu.VMEM((ffn, hidden), BF),
            pltpu.VMEM((n_tok, ffn), F32),
            pltpu.VMEM((n_stages, chunk, hidden), BF),
            pltpu.VMEM(full, BF),
            pltpu.VMEM(full[1:], BF),
            pltpu.VMEM((chunk, hidden), F32),
            dma((2,)), dma((n_stages,)), dma((n_stages,)), dma, dma((n_stages,)),
            dma((n_data - 1, n_stages)), dma((n_data - 1, n_stages)), dma((2,)),
        ],
        compiler_params=pltpu.CompilerParams(collective_id=1, has_side_effects=True, vmem_limit_bytes=VMEM_LIMIT),
        cost_estimate=pl.CostEstimate(flops=6 * n_tok * hidden * ffn * 4, bytes_accessed=4 * hidden * ffn, transcendentals=0),
        name='pipe_bwd',
    )(d_top, acts, w_in, w_out)


def wgrad_kernel(n_ref, nt_ref, d_ref, wi_ref, wo_ref, gi_ref, go_ref):
    gi_ref[...] = jnp.zeros_like(gi_ref)
    go_ref[...] = jnp.zeros_like(go_ref)
    for b in range(n_ref.shape[0] // WG_ROWS):
        rows = slice(b * WG_ROWS, (b + 1) * WG_ROWS)
        pre = jnp.dot(n_ref[rows, :], wi_ref[...], preferred_element_type=F32)
        d_act = dot(d_ref[rows, :], wo_ref[...], ((1,), (1,))).astype(BF).astype(F32)
        t = jnp.tanh(GELU_K * (pre + 0.044715 * pre * pre * pre))
        half = 0.5 * (1.0 + t)
        act = (pre * half).astype(BF)
        slope = half + 0.5 * pre * (1.0 - t * t) * (GELU_K * (1.0 + 3.0 * 0.044715 * pre * pre))
        gi_ref[...] += jnp.dot(nt_ref[:, rows], (d_act * slope).astype(BF), preferred_element_type=F32)
        go_ref[...] += dot(act, d_ref[rows, :], ((0,), (0,)))


def stage_wgrad(normed, normed_t, w_in, w_out, d_out):
    n_all, hidden = normed.shape
    ffn = w_in.shape[1]
    vmem = pl.BlockSpec(memory_space=pltpu.VMEM)
    cols = pl.BlockSpec((hidden, WG_STEP), lambda i: (0, i))
    rows = pl.BlockSpec((WG_STEP, hidden), lambda i: (i, 0))
    return pl.pallas_call(
        wgrad_kernel,
        grid=(ffn // WG_STEP,),
        in_specs=[vmem, vmem, vmem, cols, rows],
        out_specs=[cols, rows],
        out_shape=[jax.ShapeDtypeStruct((hidden, ffn), F32), jax.ShapeDtypeStruct((ffn, hidden), F32)],
        compiler_params=pltpu.CompilerParams(vmem_limit_bytes=VMEM_LIMIT),
        cost_estimate=pl.CostEstimate(flops=8 * n_all * hidden * ffn, bytes_accessed=12 * hidden * ffn, transcendentals=n_all * ffn),
        name='stage_wgrad',
    )(normed, normed_t, d_out, w_in, w_out)


def scatter_kernel(scale, firsts, starts_ref, rows_ref, perm_ref, *refs):
    pieces = refs[:-4]
    first_ref, next_ref, out_ref, upd = refs[-4:]
    tile = pl.program_id(0)
    n_tiles = pl.num_programs(0)
    owner = starts_ref[n_tiles + 1] == 1
    n_first = first_ref.shape[0]

    @pl.when(owner & (tile == 0))
    def _():
        upd[0:n_first] = first_ref[...].astype(F32) * scale
        upd[n_first:] = next_ref[...].astype(F32) * scale

    @pl.when(jnp.logical_not(owner))
    def _():
        out_ref[...] = jnp.zeros_like(out_ref)

    for q, piece in enumerate(pieces):
        @pl.when(owner & (tile >= firsts[q]) & (tile < firsts[q + 1]))
        def _():
            out_ref[...] = piece[...]

    def add_row(k, carry):
        row = rows_ref[k] - tile * TILE
        out_ref[pl.ds(row, 1), :] += upd[pl.ds(perm_ref[k], 1), :]
        return carry

    lax.fori_loop(starts_ref[tile], starts_ref[tile + 1], add_row, 0)


def scatter_plan(ids, owner, n_rows):
    n_tiles = pl.cdiv(n_rows, TILE)
    sorted_ids, perm = lax.sort((ids, lax.iota(jnp.int32, ids.shape[0])), num_keys=1)
    bounds = jnp.minimum(jnp.arange(n_tiles + 1, dtype=jnp.int32) * TILE, n_rows)
    starts = jnp.sum((ids[None, :] < bounds[:, None]).astype(jnp.int32), axis=1)
    return jnp.concatenate([starts, owner.astype(jnp.int32)[None]]), sorted_ids, perm


def scatter_rows(pieces, n_rows, first, following, plan, scale):
    hidden = first.shape[1]
    n_tiles = pl.cdiv(n_rows, TILE)
    n_upd = plan[1].shape[0]
    firsts = [0]
    for piece in pieces:
        firsts.append(firsts[-1] + piece.shape[0] // TILE)

    def piece_map(q):
        return lambda i, starts_ref, *_: (jnp.clip(i - firsts[q], 0, firsts[q + 1] - firsts[q] - 1) * starts_ref[n_tiles + 1], 0)

    vmem = pl.BlockSpec(memory_space=pltpu.VMEM)
    return pl.pallas_call(
        lambda *refs: scatter_kernel(scale, firsts, *refs),
        grid_spec=pltpu.PrefetchScalarGridSpec(
            num_scalar_prefetch=3,
            grid=(n_tiles,),
            in_specs=[pl.BlockSpec((TILE, hidden), piece_map(q)) for q in range(len(pieces))] + [vmem, vmem],
            out_specs=pl.BlockSpec((TILE, hidden), lambda i, *_: (i, 0)),
            scratch_shapes=[pltpu.VMEM((n_upd, hidden), F32)],
        ),
        out_shape=jax.ShapeDtypeStruct((n_rows, hidden), F32),
        compiler_params=pltpu.CompilerParams(vmem_limit_bytes=VMEM_LIMIT),
        name='scatter_rows',
    )(*plan, *pieces, first, following)


VTILE = 512
SHARES = (6, 6, 2, 2)
ROWS = 512
LOWEST = float(jnp.finfo(jnp.float32).min)


def head_fwd_kernel(meta, n_ref, e_ref, z_ref, top_ref, sum_ref):
    tile = pl.program_id(0)

    @pl.when(tile == 0)
    def _():
        top_ref[...] = jnp.full_like(top_ref, LOWEST)
        sum_ref[...] = jnp.zeros_like(sum_ref)

    @pl.when(tile < meta[0])
    def _():
        keep = tile * VTILE + lax.broadcasted_iota(jnp.int32, (ROWS, VTILE), 1) < meta[1]

        def block(b, carry):
            rows = pl.ds(pl.multiple_of(b * ROWS, ROWS), ROWS)
            z = dot(n_ref[rows, :], e_ref[...], ((1,), (1,)))
            z = jnp.where(keep, z, LOWEST)
            z_ref[rows, :] = z
            lanes = [z[:, k * 128:(k + 1) * 128] for k in range(VTILE // 128)]
            old = top_ref[rows, :]
            new = old
            for part in lanes:
                new = jnp.maximum(new, part)
            total = sum_ref[rows, :] * jnp.exp(old - new)
            for part in lanes:
                total = total + jnp.exp(part - new)
            top_ref[rows, :] = new
            sum_ref[rows, :] = total
            return carry

        lax.fori_loop(0, n_ref.shape[0] // ROWS, block, 0, unroll=True)


def head_fwd(meta, norm_all, table_q):
    n_all, hidden = norm_all.shape
    tiles = table_q.shape[0] // VTILE
    vmem = pl.BlockSpec(memory_space=pltpu.VMEM)
    return pl.pallas_call(
        head_fwd_kernel,
        grid_spec=pltpu.PrefetchScalarGridSpec(
            num_scalar_prefetch=1,
            grid=(tiles,),
            in_specs=[vmem, pl.BlockSpec((VTILE, hidden), lambda i, meta: (jnp.minimum(i, meta[0] - 1), 0))],
            out_specs=[pl.BlockSpec((n_all, VTILE), lambda i, meta: (0, jnp.minimum(i, meta[0] - 1))), vmem, vmem],
        ),
        out_shape=[jax.ShapeDtypeStruct((n_all, tiles * VTILE), F32)] + [jax.ShapeDtypeStruct((n_all, 128), F32)] * 2,
        compiler_params=pltpu.CompilerParams(vmem_limit_bytes=VMEM_LIMIT),
        cost_estimate=pl.CostEstimate(flops=2 * n_all * hidden * tiles * VTILE, bytes_accessed=4 * n_all * tiles * VTILE, transcendentals=n_all * tiles * VTILE),
        name='head_fwd',
    )(meta, norm_all, table_q)


def softmax_grad(z, lse, column, target, weight):
    prob = jnp.exp(z - lse)
    return (jnp.where(column == target, prob - 1.0, prob) * weight).astype(BF)


def tile_columns(tile):
    return tile * VTILE + lax.broadcasted_iota(jnp.int32, (ROWS, VTILE), 1)


def head_bwd_kernel(weight, meta, e_ref, z_ref, lse_ref, tgt_ref, dn_ref):
    tile = pl.program_id(0)

    @pl.when(tile == 0)
    def _():
        dn_ref[...] = jnp.zeros_like(dn_ref)

    @pl.when(tile < meta[0])
    def _():
        column = tile_columns(tile)
        for b in range(dn_ref.shape[0] // ROWS):
            rows = slice(b * ROWS, (b + 1) * ROWS)
            g = softmax_grad(z_ref[rows, :], lse_ref[rows, 1:2], column, tgt_ref[rows, 1:2], weight)
            dn_ref[rows, :] += jnp.dot(g, e_ref[...], preferred_element_type=F32)


def head_bwd(meta, table_q, z, lse, targets, weight):
    n_all = z.shape[0]
    hidden = table_q.shape[1]
    tiles = table_q.shape[0] // VTILE
    vmem = pl.BlockSpec(memory_space=pltpu.VMEM)
    vrows = pl.BlockSpec((VTILE, hidden), lambda i, meta: (jnp.minimum(i, meta[0] - 1), 0))
    vcols = pl.BlockSpec((n_all, VTILE), lambda i, meta: (0, jnp.minimum(i, meta[0] - 1)))
    return pl.pallas_call(
        lambda *refs: head_bwd_kernel(weight, *refs),
        grid_spec=pltpu.PrefetchScalarGridSpec(
            num_scalar_prefetch=1,
            grid=(tiles,),
            in_specs=[vrows, vcols, vmem, vmem],
            out_specs=vmem,
        ),
        out_shape=jax.ShapeDtypeStruct((n_all, hidden), F32),
        compiler_params=pltpu.CompilerParams(vmem_limit_bytes=VMEM_LIMIT),
        cost_estimate=pl.CostEstimate(flops=2 * n_all * hidden * tiles * VTILE, bytes_accessed=4 * n_all * tiles * VTILE, transcendentals=n_all * tiles * VTILE),
        name='head_bwd',
    )(meta, table_q, z, lse, targets)


def head_reduce_kernel(weights, n_stages, n_data, nm_ref, nn_ref, e_ref, zm_ref, zn_ref, lse_ref, tgt_ref, other_hbm,
                       de_ref, d_other_ref, d_mine_ref, dn, grad, pair, half_a, slot_a, slot_b,
                       l_sem, psend, precv, asend, arecv, credit):
    step_id = pl.program_id(0)
    tiles = max(SHARES)
    tile = lax.rem(step_id, tiles)
    stage = lax.axis_index('pp')
    data = lax.axis_index('dp')
    core = lax.rem(stage, 2)
    half_stage = lax.div(stage, 2)
    per = n_stages // 2
    count = n_data * per
    me = data * per + half_stage
    n_q = pair.shape[1]
    mate = (data, half_stage * 2 + 1 - core)

    def device(j):
        return (lax.div(j, per), lax.rem(j, per) * 2 + core)

    def block_of(j, side):
        return lax.div(j, per) * n_stages + lax.rem(j, per) * 2 + side

    def to_mate(src, phase, j):
        return pltpu.make_async_remote_copy(
            src_ref=src.at[block_of(j, 1 - core)], dst_ref=pair.at[j], send_sem=psend.at[phase, j], recv_sem=precv.at[phase, j],
            device_id=mate, device_id_type=MESH)

    def load_own(j):
        return pltpu.make_async_copy(other_hbm.at[block_of(j, core)], half_a.at[j], l_sem.at[j])

    def to_owner(src, dst, phase, step):
        return pltpu.make_async_remote_copy(
            src_ref=src, dst_ref=dst.at[step - 1], send_sem=asend.at[phase, step - 1], recv_sem=arecv.at[phase, step - 1],
            device_id=device(lax.rem(me + step, count)), device_id_type=MESH)

    def send_a(step):
        return to_owner(half_a.at[lax.rem(me + step, count)], slot_a, 0, step)

    def send_b(step):
        return to_owner(dn.at[block_of(lax.rem(me + step, count), core)], slot_b, 1, step)

    @pl.when(step_id == 0)
    def _():
        greet([mate] + [device(lax.rem(me + step, count)) for step in range(1, count)])
        for j in range(count):
            to_mate(other_hbm, 0, j).start()
            load_own(j).start()
        dn[...] = jnp.zeros_like(dn)

    @pl.when(step_id == 1)
    def _():
        for j in range(count):
            load_own(j).wait()
            to_mate(other_hbm, 0, j).wait()
        half_a[...] += pair[...]
        pl.semaphore_signal(credit, inc=1, device_id=mate, device_id_type=MESH)
        for step in range(1, count):
            send_a(step).start()

    @pl.when(step_id == tiles)
    def _():
        for j in range(count):
            to_mate(dn, 1, j).wait()
        for j in range(count):
            dn[block_of(j, core)] += pair[j]
        for step in range(1, count):
            send_b(step).start()

    active = tile < SHARES[0] - (SHARES[0] - SHARES[2]) * half_stage
    n_blocks = nm_ref.shape[0] // ROWS

    @pl.when(active & (step_id < tiles))
    def _():
        column = tile_columns(tile)
        per_block = ROWS // n_q
        for b in range(n_blocks):
            rows = slice(b * ROWS, (b + 1) * ROWS)
            g = softmax_grad(zm_ref[rows, :], lse_ref[rows, 0:1], column, tgt_ref[rows, 0:1], weights[0])
            part = jnp.dot(g, e_ref[...], preferred_element_type=F32)
            dn[b * per_block:(b + 1) * per_block] += part.reshape(per_block, n_q, part.shape[1])

    @pl.when(active & (step_id >= tiles))
    def _():
        column = tile_columns(tile)
        for head, (n_ref, z_ref) in enumerate(((nm_ref, zm_ref), (nn_ref, zn_ref))):
            cols = slice(head, head + 1)
            for b in range(n_blocks):
                rows = slice(b * ROWS, (b + 1) * ROWS)
                grad[rows, :] = softmax_grad(z_ref[rows, :], lse_ref[rows, cols], column, tgt_ref[rows, cols], weights[head])
            de = dot(grad[...], n_ref[...], ((0,), (0,)))
            if head == 0:
                de_ref[...] = de
            else:
                de_ref[...] += de

    @pl.when(step_id == tiles - 1)
    def _():
        pl.semaphore_wait(credit, 1)
        for j in range(count):
            to_mate(dn, 1, j).start()

    @pl.when(step_id == 2 * tiles - 1)
    def _():
        total = half_a[me]
        for step in range(1, count):
            send_a(step).wait()
            total = total + slot_a[step - 1]
        d_other_ref[...] = total
        total = dn[block_of(me, core)]
        for step in range(1, count):
            send_b(step).wait()
            total = total + slot_b[step - 1]
        d_mine_ref[...] = total


def head_reduce(norms, table_q, zs, lse, targets, weights, other, n_stages, n_data):
    n_all, hidden = norms[0].shape
    tiles = table_q.shape[0] // VTILE
    n_dev = n_stages * n_data
    n_q = n_all // n_dev
    half = n_dev // 2
    vmem = pl.BlockSpec(memory_space=pltpu.VMEM)
    single = pl.Buffered(1)
    dma = pltpu.SemaphoreType.DMA
    return pl.pallas_call(
        lambda *refs: head_reduce_kernel(weights, n_stages, n_data, *refs),
        grid=(2 * tiles,),
        in_specs=[
            vmem, vmem,
            pl.BlockSpec((VTILE, hidden), lambda i: (jnp.minimum(i, tiles - 1), 0), pipeline_mode=single),
            pl.BlockSpec((n_all, VTILE), lambda i: (0, lax.rem(i, tiles))),
            pl.BlockSpec((n_all, VTILE), lambda i: (0, jnp.maximum(i - tiles, 0)), pipeline_mode=single),
            vmem, vmem, pl.BlockSpec(memory_space=pl.ANY),
        ],
        out_specs=[pl.BlockSpec((VTILE, hidden), lambda i: (jnp.maximum(i - tiles, 0), 0)), vmem, vmem],
        out_shape=[jax.ShapeDtypeStruct(table_q.shape, F32)] + [jax.ShapeDtypeStruct((n_q, hidden), F32)] * 2,
        scratch_shapes=[
            pltpu.VMEM((n_dev, n_q, hidden), F32),
            pltpu.VMEM((n_all, VTILE), BF),
            pltpu.VMEM((half, n_q, hidden), F32),
            pltpu.VMEM((half, n_q, hidden), F32),
            pltpu.VMEM((half - 1, n_q, hidden), F32),
            pltpu.VMEM((half - 1, n_q, hidden), F32),
            dma((half,)), dma((2, half)), dma((2, half)), dma((2, half - 1)), dma((2, half - 1)),
            pltpu.SemaphoreType.REGULAR,
        ],
        compiler_params=pltpu.CompilerParams(collective_id=2, has_side_effects=True, vmem_limit_bytes=VMEM_LIMIT),
        cost_estimate=pl.CostEstimate(flops=6 * n_all * hidden * tiles * VTILE, bytes_accessed=12 * n_all * tiles * VTILE, transcendentals=3 * n_all * tiles * VTILE),
        name='head_reduce',
    )(*norms, table_q, *zs, lse, targets, other.reshape(n_dev, n_q, hidden))


def solution(mesh):
    n_stages = mesh.shape['pp']
    n_data = mesh.shape['dp']
    both = ('dp', 'pp')

    firsts = [VTILE * sum(SHARES[:q]) for q in range(n_stages + 1)]

    def from_first(pieces, stage):
        mine = jnp.where(stage == 0, pieces[0], jnp.zeros_like(pieces[0]))
        for q in range(1, n_stages):
            mine = mine + lax.ppermute(pieces[q], 'pp', [(0, q)])
        return mine

    def device_body(tokens, emb_s, w_up, w_down, gain_f, gain_h, gain_e, gain_m, w_proj, u_up, u_down):
        stage = lax.axis_index('pp')
        data = lax.axis_index('dp')
        is_first = stage == 0
        n_micro, rows_dev, width = tokens.shape
        seq_len = width - 2
        table = emb_s[0]
        v_own, hidden = table.shape
        v_dev = VTILE * max(SHARES)
        emb_scale = math.sqrt(hidden)
        w_in = w_up[0, 0]
        w_out = w_down[0, 0]
        n_seq = n_micro * rows_dev
        n_own = n_seq * seq_len
        n_all = n_own * n_data
        loss_scale = 1.0 / n_all
        q_seq = n_seq // n_stages
        n_q = q_seq * seq_len
        n_pos = n_seq * width

        tok_all = lax.all_gather(tokens.reshape(n_seq, width), 'dp', axis=0, tiled=True)
        local_ids = tok_all.reshape(-1) - data * v_own
        owned = (local_ids >= 0) & (local_ids < v_own)
        got = jnp.take(table, jnp.clip(local_ids, 0, v_own - 1), axis=0)
        got = jnp.where(owned[:, None], got, 0.0).astype(BF).reshape(n_data, n_pos, hidden)
        rows = lax.dynamic_index_in_dim(got, data, 0, keepdims=False)
        for k in range(1, n_data):
            outgoing = lax.dynamic_index_in_dim(got, lax.rem(data + k, n_data), 0, keepdims=False)
            pairs = [(d * n_stages, ((d + k) % n_data) * n_stages) for d in range(n_data)]
            rows = rows + lax.ppermute(outgoing, both, pairs)
        rows = rows.reshape(n_seq, width, hidden)

        def piece(q, source):
            part = source[firsts[q]:min(firsts[q + 1], v_own)].astype(BF)
            return jnp.pad(part, ((0, VTILE * SHARES[q] - part.shape[0]), (0, 0)))

        far = [lax.ppermute(piece(q, table), 'pp', [(0, q)]) for q in range(2, n_stages)]
        rows_q = from_first([rows[q * q_seq:(q + 1) * q_seq] for q in range(n_stages)], stage)

        first_in = (rows[:, 0:seq_len].astype(F32) * emb_scale).astype(BF).reshape(n_own, hidden)
        stage_in, hid_q = pipe_fwd(first_in, w_in, w_out, n_stages)
        table_late, stage_in = lax.optimization_barrier((table, stage_in))
        table_q = jnp.where(is_first, piece(0, table_late), 0)
        for sent in [lax.ppermute(piece(1, table_late), 'pp', [(0, 1)])] + far:
            table_q = table_q + jnp.pad(sent, ((0, v_dev - sent.shape[0]), (0, 0)))
        mtp_rows = (rows_q[:, 1:seq_len + 1].astype(F32) * emb_scale).astype(BF).reshape(n_q, hidden)

        def heads(hid, mtp):
            return normed_heads(hid, mtp, gain_f, gain_h, gain_e, gain_m, w_proj, u_up, u_down)

        (main_q, next_q), heads_back = jax.vjp(heads, hid_q, mtp_rows)

        shard_first = jnp.asarray(firsts[:-1], jnp.int32)[stage]
        shard_last = jnp.minimum(jnp.asarray(firsts[1:], jnp.int32)[stage], v_own)
        valid = shard_last - shard_first
        meta = jnp.stack([jnp.asarray(SHARES, jnp.int32)[stage], valid])

        def targets_of(ids):
            local = ids - data_base
            return jnp.where((local >= 0) & (local < valid), local, -1)

        data_base = data * v_own + shard_first

        mid_all = tok_all[:, 1:seq_len + 1].reshape(n_all)
        out_all = tok_all[:, 2:seq_len + 2].reshape(n_all)
        main_all = lax.all_gather(main_q, both, axis=0, tiled=True)
        next_all = lax.all_gather(next_q, both, axis=0, tiled=True)
        stage_in_late, next_all = lax.optimization_barrier((stage_in, next_all))
        acts_all = lax.all_gather(stage_in_late, 'dp', axis=0, tiled=True)
        main_z, main_top, main_sum = head_fwd(meta, main_all, table_q)
        next_z, next_top, next_sum = head_fwd(meta, next_all, table_q)
        lane_top = jnp.stack([main_top, next_top])
        top = jnp.max(lane_top, axis=-1)
        total = jnp.sum(jnp.stack([main_sum, next_sum]) * jnp.exp(lane_top - top[..., None]), axis=-1)
        mid_rows = rows_q[:, 1:seq_len + 1].reshape(n_q, hidden).astype(F32)
        out_rows = rows_q[:, 2:seq_len + 2].reshape(n_q, hidden).astype(F32)
        main_pick = jnp.sum(main_q.astype(F32) * mid_rows, axis=-1)
        next_pick = jnp.sum(next_q.astype(F32) * out_rows, axis=-1)
        packed = jnp.concatenate([top.reshape(-1), total.reshape(-1), main_pick, next_pick])
        packed = lax.all_gather(packed, both, axis=0)
        n_dev = n_stages * n_data
        stats = packed[:, :4 * n_all].reshape(n_dev, 2, 2, n_all)
        picks = packed[:, 4 * n_all:].reshape(n_dev, 2, n_q)
        top_all = jnp.max(stats[:, 0], axis=0)
        sum_all = jnp.sum(stats[:, 1] * jnp.exp(stats[:, 0] - top_all[None]), axis=0)
        main_lse, next_lse = jnp.log(sum_all) + top_all
        terms = jnp.sum(jnp.stack([main_lse, next_lse]), axis=-1) - jnp.sum(picks, axis=(0, 2))
        loss = (terms[0] + MTP_WEIGHT * terms[1]) * loss_scale
        lse_cols = jnp.stack([main_lse, next_lse], axis=-1)
        target_cols = jnp.stack([targets_of(mid_all), targets_of(out_all)], axis=-1)
        weights = (loss_scale, MTP_WEIGHT * loss_scale)
        next_part = head_bwd(meta, table_q, next_z, lse_cols, target_cols, weights[1])
        g_table, d_next, d_main = head_reduce((main_all, next_all), table_q, (main_z, next_z), lse_cols, target_cols, weights, next_part, n_stages, n_data)
        d_next = d_next.astype(BF)
        d_main = d_main.astype(BF)

        d_hid_q, d_rows_q = heads_back((d_main, d_next))
        d_rows_all = lax.all_gather(d_rows_q, both, axis=0, tiled=True)

        look_ids = jnp.concatenate([tok_all[:, 0:seq_len].reshape(-1), mid_all]) - data * v_own
        look_ids = jnp.where(is_first & (look_ids >= 0) & (look_ids < v_own), look_ids, v_own)
        plan = scatter_plan(look_ids, is_first, v_own)
        normed = norm_bf16(acts_all)
        prepared = lax.optimization_barrier((d_hid_q, normed, normed.T, plan))
        d_hid_q, normed, normed_t, plan = prepared
        d_out_all, d_first_all = pipe_bwd(d_hid_q, stage_in, w_in, w_out, n_stages, n_data)
        g_late, d_out_all, d_first_all = lax.optimization_barrier((g_table, d_out_all, d_first_all))
        pieces = [g_table] + [lax.ppermute(g_late[0:VTILE * SHARES[q]], 'pp', [(q, 0)]) for q in range(1, n_stages)]
        d_out_all = d_out_all.reshape(n_all, hidden)
        d_first_all = lax.all_gather(d_first_all.reshape(n_own, hidden), 'dp', axis=0, tiled=True)
        g_in, g_out = stage_wgrad(normed, normed_t, w_in, w_out, d_out_all)

        d_first_all, g_in = lax.optimization_barrier((d_first_all, g_in))
        g_shard = scatter_rows(pieces, v_own, d_first_all, d_rows_all, plan, emb_scale)
        return loss, g_shard[None], g_in[None, None], g_out[None, None]

    return jax.shard_map(device_body, mesh=mesh, in_specs=(P(None, 'dp', None), P('pp', 'dp', None), P('pp'), P('pp'), P(), P(), P(), P(), P(), P(), P()), out_specs=(P(), P('pp', 'dp', None), P('pp'), P('pp')), check_vma=False)
```

```python
import math
import jax
import jax.numpy as jnp
from jax import lax
from jax.experimental import pallas as pl
from jax.experimental.pallas import tpu as pltpu
from jax.sharding import PartitionSpec as P

MTP_WEIGHT = 0.3
EPS = 1e-6
BF = jnp.bfloat16
F32 = jnp.float32


def norm_only(acts):
    acts_f = acts.astype(F32)
    return acts_f * lax.rsqrt(jnp.mean(acts_f * acts_f, axis=-1, keepdims=True) + EPS)


def norm_bf16(acts):
    return norm_only(acts).astype(BF)


def plain_gain_norm(acts, gain):
    return (norm_only(acts) * gain.astype(F32)).astype(BF)


@jax.custom_vjp
def gain_norm(acts, gain):
    return plain_gain_norm(acts, gain)


def gain_norm_fwd(acts, gain):
    return plain_gain_norm(acts, gain), (acts, gain)


def gain_norm_bwd(saved, grad):
    return jax.vjp(plain_gain_norm, *saved)[1](lax.optimization_barrier(grad))


gain_norm.defvjp(gain_norm_fwd, gain_norm_bwd)


def gelu_bf16(pre_act):
    return jax.nn.gelu(pre_act).astype(BF)


def dot(a, b, dims):
    return lax.dot_general(a, b, (dims, ((), ())), preferred_element_type=F32)


def normed_heads(hid, rows, gain_f, gain_h, gain_e, gain_m, w_proj, u_up, u_down):
    main = gain_norm(hid, gain_f)
    joined = jnp.concatenate([gain_norm(hid, gain_h), gain_norm(rows, gain_e)], axis=-1)
    state = jnp.dot(joined, w_proj, preferred_element_type=F32).astype(BF)
    inner = gelu_bf16(jnp.dot(gain_norm(state, gain_m), u_up, preferred_element_type=F32))
    state = (state.astype(F32) + jnp.dot(inner, u_down, preferred_element_type=F32)).astype(BF)
    return main, gain_norm(state, gain_f)


MESH = pl.DeviceIdType.MESH
VMEM_LIMIT = 64 * 1024 * 1024 - 65536
FF_STEP = 2048
WG_STEP = 512
WG_ROWS = 512
TILE = 256
GELU_K = math.sqrt(2.0 / math.pi)


def gelu_slope(x):
    t = jnp.tanh(GELU_K * (x + 0.044715 * x * x * x))
    return 0.5 * (1.0 + t) + 0.5 * x * (1.0 - t * t) * (GELU_K * (1.0 + 3.0 * 0.044715 * x * x))


def greet(peers):
    barrier = pltpu.get_barrier_semaphore()
    for peer in peers:
        pl.semaphore_signal(barrier, inc=1, device_id=peer, device_id_type=MESH)
    pl.semaphore_wait(barrier, len(peers))


def pipe_fwd_kernel(n_stages, x_ref, wi_hbm, wo_hbm, in_ref, hid_ref, wi, wo, recv, send, hid_buf, acc, w_sem, send_sem, recv_sem, hsend_sem, hrecv_sem):
    stage = lax.axis_index('pp')
    data = lax.axis_index('dp')
    last = n_stages - 1
    chunk = send.shape[1]
    ffn = wi.shape[1]
    load_in = pltpu.make_async_copy(wi_hbm, wi, w_sem.at[0])
    load_out = pltpu.make_async_copy(wo_hbm, wo, w_sem.at[1])
    load_in.start()
    load_out.start()
    greet([(data, lax.rem(stage + k, n_stages)) for k in range(1, n_stages)])

    def onward(c):
        return pltpu.make_async_remote_copy(
            src_ref=send.at[c], dst_ref=recv.at[c], send_sem=send_sem.at[c], recv_sem=recv_sem.at[c],
            device_id=(data, lax.rem(stage + 1, n_stages)), device_id_type=MESH)

    def deliver(c):
        return pltpu.make_async_remote_copy(
            src_ref=send.at[c], dst_ref=hid_buf, send_sem=hsend_sem.at[c], recv_sem=hrecv_sem,
            device_id=(data, c), device_id_type=MESH)

    load_in.wait()
    load_out.wait()

    def step(c, carry):
        rows = pl.ds(pl.multiple_of(c * chunk, chunk), chunk)

        @pl.when(stage == 0)
        def _():
            in_ref[rows, :] = x_ref[rows, :]

        @pl.when(stage > 0)
        def _():
            onward(c).wait_recv()
            in_ref[rows, :] = recv[c]

        acts = in_ref[rows, :].astype(F32)
        normed = norm_only(acts).astype(BF)
        acc[...] = acts

        def ffn_step(t, inner):
            cols = pl.ds(pl.multiple_of(t * FF_STEP, FF_STEP), FF_STEP)
            pre = jnp.dot(normed, wi[:, cols], preferred_element_type=F32)
            acc[...] += jnp.dot(gelu_bf16(pre), wo[cols, :], preferred_element_type=F32)
            return inner

        lax.fori_loop(0, ffn // FF_STEP, ffn_step, 0)
        send[c] = acc[...].astype(BF)

        @pl.when(stage < last)
        def _():
            onward(c).start()

        @pl.when((stage == last) & (c < last))
        def _():
            deliver(c).start()

        return carry

    lax.fori_loop(0, n_stages, step, 0)

    @pl.when(stage < last)
    def _():
        for c in range(n_stages):
            onward(c).wait_send()
        deliver(0).wait_recv()
        hid_ref[...] = hid_buf[...]

    @pl.when(stage == last)
    def _():
        hid_ref[...] = send[last]
        for c in range(last):
            deliver(c).wait_send()


def pipe_fwd(x, w_in, w_out, n_stages):
    n_tok, hidden = x.shape
    ffn = w_in.shape[1]
    chunk = n_tok // n_stages
    vmem = pl.BlockSpec(memory_space=pltpu.VMEM)
    hbm = pl.BlockSpec(memory_space=pl.ANY)
    return pl.pallas_call(
        lambda *refs: pipe_fwd_kernel(n_stages, *refs),
        in_specs=[vmem, hbm, hbm],
        out_specs=[vmem, vmem],
        out_shape=[jax.ShapeDtypeStruct((n_tok, hidden), BF), jax.ShapeDtypeStruct((chunk, hidden), BF)],
        scratch_shapes=[
            pltpu.VMEM((hidden, ffn), BF),
            pltpu.VMEM((ffn, hidden), BF),
            pltpu.VMEM((n_stages, chunk, hidden), BF),
            pltpu.VMEM((n_stages, chunk, hidden), BF),
            pltpu.VMEM((chunk, hidden), BF),
            pltpu.VMEM((chunk, hidden), F32),
            pltpu.SemaphoreType.DMA((2,)),
            pltpu.SemaphoreType.DMA((n_stages,)),
            pltpu.SemaphoreType.DMA((n_stages,)),
            pltpu.SemaphoreType.DMA((n_stages,)),
            pltpu.SemaphoreType.DMA,
        ],
        compiler_params=pltpu.CompilerParams(collective_id=0, has_side_effects=True, vmem_limit_bytes=VMEM_LIMIT),
        cost_estimate=pl.CostEstimate(flops=4 * n_tok * hidden * ffn * 4, bytes_accessed=4 * hidden * ffn, transcendentals=0),
        name='pipe_fwd',
    )(x, w_in, w_out)


def pipe_bwd_kernel(n_stages, n_data, top_ref, acts_ref, wi_hbm, wo_hbm, dall_hbm, fall_hbm, wi, wo, slope, top, dall, fall, acc,
                    w_sem, csend, crecv, tsend, trecv, gsend, grecv, o_sem):
    stage = lax.axis_index('pp')
    data = lax.axis_index('dp')
    last = n_stages - 1
    chunk = top.shape[1]
    ffn = wi.shape[1]
    load_in = pltpu.make_async_copy(wi_hbm, wi, w_sem.at[0])
    load_out = pltpu.make_async_copy(wo_hbm, wo, w_sem.at[1])
    load_in.start()
    load_out.start()
    greet([(data, lax.rem(stage + k, n_stages)) for k in range(1, n_stages)]
          + [(lax.rem(data + k, n_data), stage) for k in range(1, n_data)])

    def hand_in(slot):
        return pltpu.make_async_remote_copy(
            src_ref=top_ref, dst_ref=top.at[slot], send_sem=tsend, recv_sem=trecv.at[slot],
            device_id=(data, last), device_id_type=MESH)

    def back(c):
        return pltpu.make_async_remote_copy(
            src_ref=fall.at[c], dst_ref=dall.at[data, c], send_sem=csend.at[c], recv_sem=crecv.at[c],
            device_id=(data, lax.rem(stage + last, n_stages)), device_id_type=MESH)

    def share(buf, owner, k, c, send_sem, recv_sem):
        return pltpu.make_async_remote_copy(
            src_ref=buf.at[owner, c], dst_ref=buf.at[owner, c], send_sem=send_sem.at[k - 1, c], recv_sem=recv_sem.at[k - 1, c],
            device_id=(lax.rem(data + k, n_data), stage), device_id_type=MESH)

    @pl.when(stage < last)
    def _():
        hand_in(stage).start()

    @pl.when(stage == last)
    def _():
        top[last] = top_ref[...]

    load_in.wait()
    normed_all = norm_only(acts_ref[...].astype(F32)).astype(BF)

    def slope_step(t, carry):
        cols = pl.ds(pl.multiple_of(t * FF_STEP, FF_STEP), FF_STEP)
        slope[:, cols] = gelu_slope(jnp.dot(normed_all, wi[:, cols], preferred_element_type=F32))
        return carry

    lax.fori_loop(0, ffn // FF_STEP, slope_step, 0)
    load_out.wait()

    def step(c, carry):
        rows = pl.ds(pl.multiple_of(c * chunk, chunk), chunk)

        @pl.when((stage == last) & (c < last))
        def _():
            hand_in(c).wait_recv()

        @pl.when(stage == last)
        def _():
            dall[data, c] = top[c]

        @pl.when(stage < last)
        def _():
            back(c).wait_recv()

        d_out = dall[data, c]
        acc[...] = jnp.zeros_like(acc)

        def ffn_step(t, inner):
            cols = pl.ds(pl.multiple_of(t * FF_STEP, FF_STEP), FF_STEP)
            d_act = dot(d_out, wo[cols, :], ((1,), (1,))).astype(BF).astype(F32)
            d_pre = (d_act * slope[rows, cols]).astype(BF)
            acc[...] += dot(d_pre, wi[:, cols], ((1,), (1,)))
            return inner

        lax.fori_loop(0, ffn // FF_STEP, ffn_step, 0)
        d_norm = acc[...].astype(BF).astype(F32)
        acts = acts_ref[rows, :].astype(F32)
        scale = lax.rsqrt(jnp.mean(acts * acts, axis=-1, keepdims=True) + EPS)
        inner_mean = jnp.mean(d_norm * acts, axis=-1, keepdims=True)
        d_acts = (d_norm * scale - acts * (scale * scale * scale * inner_mean)).astype(BF)
        fall[c] = (d_out.astype(F32) + d_acts.astype(F32)).astype(BF)

        @pl.when(stage > 0)
        def _():
            back(c).start()

        for k in range(1, n_data):
            share(dall, data, k, c, gsend, grecv).start()

        return carry

    lax.fori_loop(0, n_stages, step, 0)

    @pl.when(stage < last)
    def _():
        hand_in(stage).wait_send()

    @pl.when(stage > 0)
    def _():
        for c in range(n_stages):
            back(c).wait_send()

    for k in range(1, n_data):
        for c in range(n_stages):
            share(dall, data, k, c, gsend, grecv).wait_send()
            share(dall, lax.rem(data + n_data - k, n_data), k, c, gsend, grecv).wait_recv()
    save = pltpu.make_async_copy(dall, dall_hbm, o_sem.at[0])
    save.start()

    save_first = pltpu.make_async_copy(fall, fall_hbm, o_sem.at[1])
    save_first.start()
    save_first.wait()
    save.wait()


def pipe_bwd(d_top, acts, w_in, w_out, n_stages, n_data):
    n_tok, hidden = acts.shape
    ffn = w_in.shape[1]
    chunk = n_tok // n_stages
    vmem = pl.BlockSpec(memory_space=pltpu.VMEM)
    hbm = pl.BlockSpec(memory_space=pl.ANY)
    full = (n_data, n_stages, chunk, hidden)
    dma = pltpu.SemaphoreType.DMA
    return pl.pallas_call(
        lambda *refs: pipe_bwd_kernel(n_stages, n_data, *refs),
        in_specs=[vmem, vmem, hbm, hbm],
        out_specs=[hbm, hbm],
        out_shape=[jax.ShapeDtypeStruct(full, BF), jax.ShapeDtypeStruct(full[1:], BF)],
        scratch_shapes=[
            pltpu.VMEM((hidden, ffn), BF),
            pltpu.VMEM((ffn, hidden), BF),
            pltpu.VMEM((n_tok, ffn), F32),
            pltpu.VMEM((n_stages, chunk, hidden), BF),
            pltpu.VMEM(full, BF),
            pltpu.VMEM(full[1:], BF),
            pltpu.VMEM((chunk, hidden), F32),
            dma((2,)), dma((n_stages,)), dma((n_stages,)), dma, dma((n_stages,)),
            dma((n_data - 1, n_stages)), dma((n_data - 1, n_stages)), dma((2,)),
        ],
        compiler_params=pltpu.CompilerParams(collective_id=1, has_side_effects=True, vmem_limit_bytes=VMEM_LIMIT),
        cost_estimate=pl.CostEstimate(flops=6 * n_tok * hidden * ffn * 4, bytes_accessed=4 * hidden * ffn, transcendentals=0),
        name='pipe_bwd',
    )(d_top, acts, w_in, w_out)


def wgrad_kernel(acts_ref, d_ref, wi_ref, wo_ref, gi_ref, go_ref, n_ref, nt_ref):
    @pl.when(pl.program_id(0) == 0)
    def _():
        for b in range(n_ref.shape[0] // WG_ROWS):
            rows = slice(b * WG_ROWS, (b + 1) * WG_ROWS)
            normed = norm_bf16(acts_ref[rows, :])
            n_ref[rows, :] = normed
            nt_ref[:, rows] = normed.T

    gi_ref[...] = jnp.zeros_like(gi_ref)
    go_ref[...] = jnp.zeros_like(go_ref)
    for b in range(n_ref.shape[0] // WG_ROWS):
        rows = slice(b * WG_ROWS, (b + 1) * WG_ROWS)
        pre = jnp.dot(n_ref[rows, :], wi_ref[...], preferred_element_type=F32)
        d_act = dot(d_ref[rows, :], wo_ref[...], ((1,), (1,))).astype(BF).astype(F32)
        t = jnp.tanh(GELU_K * (pre + 0.044715 * pre * pre * pre))
        half = 0.5 * (1.0 + t)
        act = (pre * half).astype(BF)
        slope = half + 0.5 * pre * (1.0 - t * t) * (GELU_K * (1.0 + 3.0 * 0.044715 * pre * pre))
        gi_ref[...] += jnp.dot(nt_ref[:, rows], (d_act * slope).astype(BF), preferred_element_type=F32)
        go_ref[...] += dot(act, d_ref[rows, :], ((0,), (0,)))


def stage_wgrad(acts, w_in, w_out, d_out):
    n_all, hidden = acts.shape
    ffn = w_in.shape[1]
    vmem = pl.BlockSpec(memory_space=pltpu.VMEM)
    cols = pl.BlockSpec((hidden, WG_STEP), lambda i: (0, i))
    rows = pl.BlockSpec((WG_STEP, hidden), lambda i: (i, 0))
    return pl.pallas_call(
        wgrad_kernel,
        grid=(ffn // WG_STEP,),
        in_specs=[vmem, vmem, cols, rows],
        out_specs=[cols, rows],
        scratch_shapes=[pltpu.VMEM((n_all, hidden), BF), pltpu.VMEM((hidden, n_all), BF)],
        out_shape=[jax.ShapeDtypeStruct((hidden, ffn), F32), jax.ShapeDtypeStruct((ffn, hidden), F32)],
        compiler_params=pltpu.CompilerParams(vmem_limit_bytes=VMEM_LIMIT),
        cost_estimate=pl.CostEstimate(flops=8 * n_all * hidden * ffn, bytes_accessed=12 * hidden * ffn, transcendentals=n_all * ffn),
        name='stage_wgrad',
    )(acts, d_out, w_in, w_out)


def scatter_kernel(scale, firsts, starts_ref, rows_ref, perm_ref, *refs):
    pieces = refs[:-4]
    first_ref, next_ref, out_ref, upd = refs[-4:]
    tile = pl.program_id(0)
    n_tiles = pl.num_programs(0)
    owner = starts_ref[n_tiles + 1] == 1
    n_first = first_ref.shape[0]

    @pl.when(owner & (tile == 0))
    def _():
        upd[0:n_first] = first_ref[...].astype(F32) * scale
        upd[n_first:] = next_ref[...].astype(F32) * scale

    @pl.when(jnp.logical_not(owner))
    def _():
        out_ref[...] = jnp.zeros_like(out_ref)

    for q, piece in enumerate(pieces):
        @pl.when(owner & (tile >= firsts[q]) & (tile < firsts[q + 1]))
        def _():
            out_ref[...] = piece[...]

    def add_row(k, carry):
        row = rows_ref[k] - tile * TILE
        out_ref[pl.ds(row, 1), :] += upd[pl.ds(perm_ref[k], 1), :]
        return carry

    lax.fori_loop(starts_ref[tile], starts_ref[tile + 1], add_row, 0)


def scatter_plan(ids, owner, n_rows):
    n_tiles = pl.cdiv(n_rows, TILE)
    sorted_ids, perm = lax.sort((ids, lax.iota(jnp.int32, ids.shape[0])), num_keys=1)
    bounds = jnp.minimum(jnp.arange(n_tiles + 1, dtype=jnp.int32) * TILE, n_rows)
    starts = jnp.sum((ids[None, :] < bounds[:, None]).astype(jnp.int32), axis=1)
    return jnp.concatenate([starts, owner.astype(jnp.int32)[None]]), sorted_ids, perm


def scatter_rows(pieces, n_rows, first, following, plan, scale):
    hidden = first.shape[1]
    n_tiles = pl.cdiv(n_rows, TILE)
    n_upd = plan[1].shape[0]
    firsts = [0]
    for piece in pieces:
        firsts.append(firsts[-1] + piece.shape[0] // TILE)

    def piece_map(q):
        return lambda i, starts_ref, *_: (jnp.clip(i - firsts[q], 0, firsts[q + 1] - firsts[q] - 1) * starts_ref[n_tiles + 1], 0)

    vmem = pl.BlockSpec(memory_space=pltpu.VMEM)
    return pl.pallas_call(
        lambda *refs: scatter_kernel(scale, firsts, *refs),
        grid_spec=pltpu.PrefetchScalarGridSpec(
            num_scalar_prefetch=3,
            grid=(n_tiles,),
            in_specs=[pl.BlockSpec((TILE, hidden), piece_map(q)) for q in range(len(pieces))] + [vmem, vmem],
            out_specs=pl.BlockSpec((TILE, hidden), lambda i, *_: (i, 0)),
            scratch_shapes=[pltpu.VMEM((n_upd, hidden), F32)],
        ),
        out_shape=jax.ShapeDtypeStruct((n_rows, hidden), F32),
        compiler_params=pltpu.CompilerParams(vmem_limit_bytes=VMEM_LIMIT),
        name='scatter_rows',
    )(*plan, *pieces, first, following)


VTILE = 512
SHARES = (6, 6, 2, 2)
ROWS = 512
LOWEST = float(jnp.finfo(jnp.float32).min)


def head_fwd_kernel(meta, n_ref, e_ref, z_ref, top_ref, sum_ref):
    tile = pl.program_id(0)

    @pl.when(tile == 0)
    def _():
        top_ref[...] = jnp.full_like(top_ref, LOWEST)
        sum_ref[...] = jnp.zeros_like(sum_ref)

    @pl.when(tile < meta[0])
    def _():
        keep = tile * VTILE + lax.broadcasted_iota(jnp.int32, (ROWS, VTILE), 1) < meta[1]

        def block(b, carry):
            rows = pl.ds(pl.multiple_of(b * ROWS, ROWS), ROWS)
            z = dot(n_ref[rows, :], e_ref[...], ((1,), (1,)))
            z = jnp.where(keep, z, LOWEST)
            z_ref[rows, :] = z
            lanes = [z[:, k * 128:(k + 1) * 128] for k in range(VTILE // 128)]
            old = top_ref[rows, :]
            new = old
            for part in lanes:
                new = jnp.maximum(new, part)
            total = sum_ref[rows, :] * jnp.exp(old - new)
            for part in lanes:
                total = total + jnp.exp(part - new)
            top_ref[rows, :] = new
            sum_ref[rows, :] = total
            return carry

        lax.fori_loop(0, n_ref.shape[0] // ROWS, block, 0, unroll=True)


def head_fwd(meta, norm_all, table_q):
    n_all, hidden = norm_all.shape
    tiles = table_q.shape[0] // VTILE
    vmem = pl.BlockSpec(memory_space=pltpu.VMEM)
    return pl.pallas_call(
        head_fwd_kernel,
        grid_spec=pltpu.PrefetchScalarGridSpec(
            num_scalar_prefetch=1,
            grid=(tiles,),
            in_specs=[vmem, pl.BlockSpec((VTILE, hidden), lambda i, meta: (jnp.minimum(i, meta[0] - 1), 0))],
            out_specs=[pl.BlockSpec((n_all, VTILE), lambda i, meta: (0, jnp.minimum(i, meta[0] - 1))), vmem, vmem],
        ),
        out_shape=[jax.ShapeDtypeStruct((n_all, tiles * VTILE), F32)] + [jax.ShapeDtypeStruct((n_all, 128), F32)] * 2,
        compiler_params=pltpu.CompilerParams(vmem_limit_bytes=VMEM_LIMIT),
        cost_estimate=pl.CostEstimate(flops=2 * n_all * hidden * tiles * VTILE, bytes_accessed=4 * n_all * tiles * VTILE, transcendentals=n_all * tiles * VTILE),
        name='head_fwd',
    )(meta, norm_all, table_q)


def softmax_grad(z, lse, column, target, weight):
    prob = jnp.exp(z - lse)
    return (jnp.where(column == target, prob - 1.0, prob) * weight).astype(BF)


def tile_columns(tile):
    return tile * VTILE + lax.broadcasted_iota(jnp.int32, (ROWS, VTILE), 1)


def head_bwd_kernel(weight, meta, e_ref, z_ref, lse_ref, tgt_ref, dn_ref):
    tile = pl.program_id(0)

    @pl.when(tile == 0)
    def _():
        dn_ref[...] = jnp.zeros_like(dn_ref)

    @pl.when(tile < meta[0])
    def _():
        column = tile_columns(tile)
        for b in range(dn_ref.shape[0] // ROWS):
            rows = slice(b * ROWS, (b + 1) * ROWS)
            g = softmax_grad(z_ref[rows, :], lse_ref[rows, 1:2], column, tgt_ref[rows, 1:2], weight)
            dn_ref[rows, :] += jnp.dot(g, e_ref[...], preferred_element_type=F32)


def head_bwd(meta, table_q, z, lse, targets, weight):
    n_all = z.shape[0]
    hidden = table_q.shape[1]
    tiles = table_q.shape[0] // VTILE
    vmem = pl.BlockSpec(memory_space=pltpu.VMEM)
    vrows = pl.BlockSpec((VTILE, hidden), lambda i, meta: (jnp.minimum(i, meta[0] - 1), 0))
    vcols = pl.BlockSpec((n_all, VTILE), lambda i, meta: (0, jnp.minimum(i, meta[0] - 1)))
    return pl.pallas_call(
        lambda *refs: head_bwd_kernel(weight, *refs),
        grid_spec=pltpu.PrefetchScalarGridSpec(
            num_scalar_prefetch=1,
            grid=(tiles,),
            in_specs=[vrows, vcols, vmem, vmem],
            out_specs=vmem,
        ),
        out_shape=jax.ShapeDtypeStruct((n_all, hidden), F32),
        compiler_params=pltpu.CompilerParams(vmem_limit_bytes=VMEM_LIMIT),
        cost_estimate=pl.CostEstimate(flops=2 * n_all * hidden * tiles * VTILE, bytes_accessed=4 * n_all * tiles * VTILE, transcendentals=n_all * tiles * VTILE),
        name='head_bwd',
    )(meta, table_q, z, lse, targets)


def head_reduce_kernel(weights, n_stages, n_data, nm_ref, nn_ref, e_ref, zm_ref, zn_ref, lse_ref, tgt_ref, other_hbm,
                       de_ref, d_other_ref, d_mine_ref, dn, grad, pair, half_a, slot_a, slot_b,
                       l_sem, psend, precv, asend, arecv, credit):
    step_id = pl.program_id(0)
    tiles = max(SHARES)
    tile = lax.rem(step_id, tiles)
    stage = lax.axis_index('pp')
    data = lax.axis_index('dp')
    core = lax.rem(stage, 2)
    half_stage = lax.div(stage, 2)
    per = n_stages // 2
    count = n_data * per
    me = data * per + half_stage
    n_q = pair.shape[1]
    mate = (data, half_stage * 2 + 1 - core)

    def device(j):
        return (lax.div(j, per), lax.rem(j, per) * 2 + core)

    def block_of(j, side):
        return lax.div(j, per) * n_stages + lax.rem(j, per) * 2 + side

    def to_mate(src, phase, j):
        return pltpu.make_async_remote_copy(
            src_ref=src.at[block_of(j, 1 - core)], dst_ref=pair.at[j], send_sem=psend.at[phase, j], recv_sem=precv.at[phase, j],
            device_id=mate, device_id_type=MESH)

    def load_own(j):
        return pltpu.make_async_copy(other_hbm.at[block_of(j, core)], half_a.at[j], l_sem.at[j])

    def to_owner(src, dst, phase, step):
        return pltpu.make_async_remote_copy(
            src_ref=src, dst_ref=dst.at[step - 1], send_sem=asend.at[phase, step - 1], recv_sem=arecv.at[phase, step - 1],
            device_id=device(lax.rem(me + step, count)), device_id_type=MESH)

    def send_a(step):
        return to_owner(half_a.at[lax.rem(me + step, count)], slot_a, 0, step)

    def send_b(step):
        return to_owner(dn.at[block_of(lax.rem(me + step, count), core)], slot_b, 1, step)

    @pl.when(step_id == 0)
    def _():
        greet([mate] + [device(lax.rem(me + step, count)) for step in range(1, count)])
        for j in range(count):
            to_mate(other_hbm, 0, j).start()
            load_own(j).start()
        dn[...] = jnp.zeros_like(dn)

    @pl.when(step_id == 1)
    def _():
        for j in range(count):
            load_own(j).wait()
            to_mate(other_hbm, 0, j).wait()
        half_a[...] += pair[...]
        pl.semaphore_signal(credit, inc=1, device_id=mate, device_id_type=MESH)
        for step in range(1, count):
            send_a(step).start()

    @pl.when(step_id == tiles)
    def _():
        for j in range(count):
            to_mate(dn, 1, j).wait()
        for j in range(count):
            dn[block_of(j, core)] += pair[j]
        for step in range(1, count):
            send_b(step).start()

    active = tile < SHARES[0] - (SHARES[0] - SHARES[2]) * half_stage
    n_blocks = nm_ref.shape[0] // ROWS

    @pl.when(active & (step_id < tiles))
    def _():
        column = tile_columns(tile)
        per_block = ROWS // n_q
        for b in range(n_blocks):
            rows = slice(b * ROWS, (b + 1) * ROWS)
            g = softmax_grad(zm_ref[rows, :], lse_ref[rows, 0:1], column, tgt_ref[rows, 0:1], weights[0])
            part = jnp.dot(g, e_ref[...], preferred_element_type=F32)
            dn[b * per_block:(b + 1) * per_block] += part.reshape(per_block, n_q, part.shape[1])

    @pl.when(active & (step_id >= tiles))
    def _():
        column = tile_columns(tile)
        for head, (n_ref, z_ref) in enumerate(((nm_ref, zm_ref), (nn_ref, zn_ref))):
            cols = slice(head, head + 1)
            for b in range(n_blocks):
                rows = slice(b * ROWS, (b + 1) * ROWS)
                grad[rows, :] = softmax_grad(z_ref[rows, :], lse_ref[rows, cols], column, tgt_ref[rows, cols], weights[head])
            de = dot(grad[...], n_ref[...], ((0,), (0,)))
            if head == 0:
                de_ref[...] = de
            else:
                de_ref[...] += de

    @pl.when(step_id == tiles - 1)
    def _():
        pl.semaphore_wait(credit, 1)
        for j in range(count):
            to_mate(dn, 1, j).start()

    @pl.when(step_id == 2 * tiles - 1)
    def _():
        total = half_a[me]
        for step in range(1, count):
            send_a(step).wait()
            total = total + slot_a[step - 1]
        d_other_ref[...] = total
        total = dn[block_of(me, core)]
        for step in range(1, count):
            send_b(step).wait()
            total = total + slot_b[step - 1]
        d_mine_ref[...] = total


def head_reduce(norms, table_q, zs, lse, targets, weights, other, n_stages, n_data):
    n_all, hidden = norms[0].shape
    tiles = table_q.shape[0] // VTILE
    n_dev = n_stages * n_data
    n_q = n_all // n_dev
    half = n_dev // 2
    vmem = pl.BlockSpec(memory_space=pltpu.VMEM)
    single = pl.Buffered(1)
    dma = pltpu.SemaphoreType.DMA
    return pl.pallas_call(
        lambda *refs: head_reduce_kernel(weights, n_stages, n_data, *refs),
        grid=(2 * tiles,),
        in_specs=[
            vmem, vmem,
            pl.BlockSpec((VTILE, hidden), lambda i: (jnp.minimum(i, tiles - 1), 0), pipeline_mode=single),
            pl.BlockSpec((n_all, VTILE), lambda i: (0, lax.rem(i, tiles))),
            pl.BlockSpec((n_all, VTILE), lambda i: (0, jnp.maximum(i - tiles, 0)), pipeline_mode=single),
            vmem, vmem, pl.BlockSpec(memory_space=pl.ANY),
        ],
        out_specs=[pl.BlockSpec((VTILE, hidden), lambda i: (jnp.maximum(i - tiles, 0), 0)), vmem, vmem],
        out_shape=[jax.ShapeDtypeStruct(table_q.shape, F32)] + [jax.ShapeDtypeStruct((n_q, hidden), F32)] * 2,
        scratch_shapes=[
            pltpu.VMEM((n_dev, n_q, hidden), F32),
            pltpu.VMEM((n_all, VTILE), BF),
            pltpu.VMEM((half, n_q, hidden), F32),
            pltpu.VMEM((half, n_q, hidden), F32),
            pltpu.VMEM((half - 1, n_q, hidden), F32),
            pltpu.VMEM((half - 1, n_q, hidden), F32),
            dma((half,)), dma((2, half)), dma((2, half)), dma((2, half - 1)), dma((2, half - 1)),
            pltpu.SemaphoreType.REGULAR,
        ],
        compiler_params=pltpu.CompilerParams(collective_id=2, has_side_effects=True, vmem_limit_bytes=VMEM_LIMIT),
        cost_estimate=pl.CostEstimate(flops=6 * n_all * hidden * tiles * VTILE, bytes_accessed=12 * n_all * tiles * VTILE, transcendentals=3 * n_all * tiles * VTILE),
        name='head_reduce',
    )(*norms, table_q, *zs, lse, targets, other.reshape(n_dev, n_q, hidden))


def solution(mesh):
    n_stages = mesh.shape['pp']
    n_data = mesh.shape['dp']
    both = ('dp', 'pp')

    firsts = [VTILE * sum(SHARES[:q]) for q in range(n_stages + 1)]

    def from_first(pieces, stage):
        mine = jnp.where(stage == 0, pieces[0], jnp.zeros_like(pieces[0]))
        for q in range(1, n_stages):
            mine = mine + lax.ppermute(pieces[q], 'pp', [(0, q)])
        return mine

    def device_body(tokens, emb_s, w_up, w_down, gain_f, gain_h, gain_e, gain_m, w_proj, u_up, u_down):
        stage = lax.axis_index('pp')
        data = lax.axis_index('dp')
        is_first = stage == 0
        n_micro, rows_dev, width = tokens.shape
        seq_len = width - 2
        table = emb_s[0]
        v_own, hidden = table.shape
        v_dev = VTILE * max(SHARES)
        emb_scale = math.sqrt(hidden)
        w_in = w_up[0, 0]
        w_out = w_down[0, 0]
        n_seq = n_micro * rows_dev
        n_own = n_seq * seq_len
        n_all = n_own * n_data
        loss_scale = 1.0 / n_all
        q_seq = n_seq // n_stages
        n_q = q_seq * seq_len
        n_pos = n_seq * width

        tok_all = lax.all_gather(tokens.reshape(n_seq, width), 'dp', axis=0, tiled=True)
        local_ids = tok_all.reshape(-1) - data * v_own
        owned = (local_ids >= 0) & (local_ids < v_own)
        got = jnp.take(table, jnp.clip(local_ids, 0, v_own - 1), axis=0)
        got = jnp.where(owned[:, None], got, 0.0).astype(BF).reshape(n_data, n_pos, hidden)
        rows = lax.dynamic_index_in_dim(got, data, 0, keepdims=False)
        for k in range(1, n_data):
            outgoing = lax.dynamic_index_in_dim(got, lax.rem(data + k, n_data), 0, keepdims=False)
            pairs = [(d * n_stages, ((d + k) % n_data) * n_stages) for d in range(n_data)]
            rows = rows + lax.ppermute(outgoing, both, pairs)
        rows = rows.reshape(n_seq, width, hidden)

        def piece(q, source):
            part = source[firsts[q]:min(firsts[q + 1], v_own)].astype(BF)
            return jnp.pad(part, ((0, VTILE * SHARES[q] - part.shape[0]), (0, 0)))

        far = [lax.ppermute(piece(q, table), 'pp', [(0, q)]) for q in range(2, n_stages)]
        rows_q = from_first([rows[q * q_seq:(q + 1) * q_seq] for q in range(n_stages)], stage)

        first_in = (rows[:, 0:seq_len].astype(F32) * emb_scale).astype(BF).reshape(n_own, hidden)
        stage_in, hid_q = pipe_fwd(first_in, w_in, w_out, n_stages)
        table_late, stage_in = lax.optimization_barrier((table, stage_in))
        table_q = jnp.where(is_first, piece(0, table_late), 0)
        for sent in [lax.ppermute(piece(1, table_late), 'pp', [(0, 1)])] + far:
            table_q = table_q + jnp.pad(sent, ((0, v_dev - sent.shape[0]), (0, 0)))
        mtp_rows = (rows_q[:, 1:seq_len + 1].astype(F32) * emb_scale).astype(BF).reshape(n_q, hidden)

        def heads(hid, mtp):
            return normed_heads(hid, mtp, gain_f, gain_h, gain_e, gain_m, w_proj, u_up, u_down)

        (main_q, next_q), heads_back = jax.vjp(heads, hid_q, mtp_rows)

        shard_first = jnp.asarray(firsts[:-1], jnp.int32)[stage]
        shard_last = jnp.minimum(jnp.asarray(firsts[1:], jnp.int32)[stage], v_own)
        valid = shard_last - shard_first
        meta = jnp.stack([jnp.asarray(SHARES, jnp.int32)[stage], valid])

        def targets_of(ids):
            local = ids - data_base
            return jnp.where((local >= 0) & (local < valid), local, -1)

        data_base = data * v_own + shard_first

        mid_all = tok_all[:, 1:seq_len + 1].reshape(n_all)
        out_all = tok_all[:, 2:seq_len + 2].reshape(n_all)
        main_all = lax.all_gather(main_q, both, axis=0, tiled=True)
        next_all = lax.all_gather(next_q, both, axis=0, tiled=True)
        stage_in_late, next_all = lax.optimization_barrier((stage_in, next_all))
        acts_all = lax.all_gather(stage_in_late, 'dp', axis=0, tiled=True)
        main_z, main_top, main_sum = head_fwd(meta, main_all, table_q)
        next_z, next_top, next_sum = head_fwd(meta, next_all, table_q)
        lane_top = jnp.stack([main_top, next_top])
        top = jnp.max(lane_top, axis=-1)
        total = jnp.sum(jnp.stack([main_sum, next_sum]) * jnp.exp(lane_top - top[..., None]), axis=-1)
        mid_rows = rows_q[:, 1:seq_len + 1].reshape(n_q, hidden).astype(F32)
        out_rows = rows_q[:, 2:seq_len + 2].reshape(n_q, hidden).astype(F32)
        main_pick = jnp.sum(main_q.astype(F32) * mid_rows, axis=-1)
        next_pick = jnp.sum(next_q.astype(F32) * out_rows, axis=-1)
        packed = jnp.concatenate([top.reshape(-1), total.reshape(-1), main_pick, next_pick])
        packed = lax.all_gather(packed, both, axis=0)
        n_dev = n_stages * n_data
        stats = packed[:, :4 * n_all].reshape(n_dev, 2, 2, n_all)
        picks = packed[:, 4 * n_all:].reshape(n_dev, 2, n_q)
        top_all = jnp.max(stats[:, 0], axis=0)
        sum_all = jnp.sum(stats[:, 1] * jnp.exp(stats[:, 0] - top_all[None]), axis=0)
        main_lse, next_lse = jnp.log(sum_all) + top_all
        terms = jnp.sum(jnp.stack([main_lse, next_lse]), axis=-1) - jnp.sum(picks, axis=(0, 2))
        loss = (terms[0] + MTP_WEIGHT * terms[1]) * loss_scale
        lse_cols = jnp.stack([main_lse, next_lse], axis=-1)
        target_cols = jnp.stack([targets_of(mid_all), targets_of(out_all)], axis=-1)
        weights = (loss_scale, MTP_WEIGHT * loss_scale)
        next_part = head_bwd(meta, table_q, next_z, lse_cols, target_cols, weights[1])
        g_table, d_next, d_main = head_reduce((main_all, next_all), table_q, (main_z, next_z), lse_cols, target_cols, weights, next_part, n_stages, n_data)
        d_next = d_next.astype(BF)
        d_main = d_main.astype(BF)

        d_hid_q, d_rows_q = heads_back((d_main, d_next))
        d_rows_all = lax.all_gather(d_rows_q, both, axis=0, tiled=True)

        look_ids = jnp.concatenate([tok_all[:, 0:seq_len].reshape(-1), mid_all]) - data * v_own
        look_ids = jnp.where(is_first & (look_ids >= 0) & (look_ids < v_own), look_ids, v_own)
        plan = scatter_plan(look_ids, is_first, v_own)
        d_hid_q, acts_all, plan = lax.optimization_barrier((d_hid_q, acts_all, plan))
        d_out_all, d_first_all = pipe_bwd(d_hid_q, stage_in, w_in, w_out, n_stages, n_data)
        g_late, d_out_all, d_first_all = lax.optimization_barrier((g_table, d_out_all, d_first_all))
        pieces = [g_table] + [lax.ppermute(g_late[0:VTILE * SHARES[q]], 'pp', [(q, 0)]) for q in range(1, n_stages)]
        d_out_all = d_out_all.reshape(n_all, hidden)
        d_first_all = lax.all_gather(d_first_all.reshape(n_own, hidden), 'dp', axis=0, tiled=True)
        g_in, g_out = stage_wgrad(acts_all, w_in, w_out, d_out_all)

        d_first_all, g_in = lax.optimization_barrier((d_first_all, g_in))
        g_shard = scatter_rows(pieces, v_own, d_first_all, d_rows_all, plan, emb_scale)
        return loss, g_shard[None], g_in[None, None], g_out[None, None]

    return jax.shard_map(device_body, mesh=mesh, in_specs=(P(None, 'dp', None), P('pp', 'dp', None), P('pp'), P('pp'), P(), P(), P(), P(), P(), P(), P()), out_specs=(P(), P('pp', 'dp', None), P('pp'), P('pp')), check_vma=False)
```
